256 devices in a mesh: seq: 16 (over y_hi, x, core), exp: 16 (over y_lo, z).
Axes of the slice: x: 4, y: 4 (y_hi: 2, y_lo: 2; y = y_hi * 2 + y_lo), z: 8, core: 2. Of those that a mesh axis runs over, the one named last changes fastest.
Arguments:
- grad_out: bfloat16 [32768, 2048], P(('seq', 'exp')), may hold values from -6 to 6
- out_proj: bfloat16 [4096, 2048], P('exp'), may hold values from -0.125 to 0.125
- step_size: float32 [64, 32768], P('exp', 'seq'), may hold values from 0.001 to 0.1
- log_decay: float32 [64, 32768], P('exp', 'seq'), may hold values from -1 to 0, as said below
- b_input: float32 [16, 32768], P(None, 'seq'), may hold values from -1.5 to 1.5
- c_output: float32 [16, 32768], P(None, 'seq'), may hold values from -1.5 to 1.5
- skip_gain: float32 [4096], P('exp'), may hold values from 0.5 to 1.5
- expert_ids: int32 [32768, 2], P('seq'), may hold values from 0 to 15, all different within a row; in each aligned block of 128 rows (0 to 127, 128 to 255, ...) at most 18 rows name the same one
- hidden_act: bfloat16 [16, 256, 18, 8192], P('exp', None, None, 'seq'), may hold values from -6 to 6
- w_down: bfloat16 [16, 8192, 2048], P('exp', 'seq'), may hold values from -0.0029296875 to 0.0029296875
Outputs:
- d_inner: bfloat16 [32768, 4096], P('seq', 'exp')
- d_gate: float32 [2, 32768], P(None, ('seq', 'exp'))
The draws below stay inside these ranges and needn't reach their ends.
Inputs may be any that keep to these rules, and one draw needn't show every extreme that they name: `expert_ids`: each row names 2 different experts. Within the rows of one token group no expert is named by more than 18 rows, and in every draw some expert is named by exactly 18 rows of some group. `log_decay`: every entry is negative.
All inputs are finite; a program needn't handle non-finite values.
Results may differ from the reference program's by a relative error of at most 0.00065.
Values may be sent and summed in bfloat16 or wider, within the bound.
A program may use at most 128 MiB of HBM per device.

```python
import math
from functools import partial
import jax
import jax.numpy as jnp
import numpy as np
from jax import lax

D = 2048
INNER = 4096
STATE = 16
HEAD = 64
FF = 8192
TOP = 2
TOK_DEV = 128
EXPERTS = 16
CAP = 18
SEQ_ROWS = 2048
SEQUENCE_ITEMS = 32768
SOURCES = 256
HEADS = 64


def draw_log_decay(key, part):
    stochastic_seeds = jax.random.split(key, 7)
    slow_rate = jnp.exp(jax.random.uniform(stochastic_seeds[0], (HEADS, 1), jnp.float32, math.log(0.1 / SEQUENCE_ITEMS), math.log(0.8 / SEQUENCE_ITEMS)))
    fast_rate = jnp.exp(jax.random.uniform(stochastic_seeds[1], (HEADS, 1), jnp.float32, math.log(0.02), math.log(0.05)))
    slow_mask = jax.random.bernoulli(stochastic_seeds[2], 0.5, (HEADS, 1))
    per_channel_forgetting = jnp.where(slow_mask, slow_rate, fast_rate)
    forgetting_noise = jnp.exp(jax.random.uniform(stochastic_seeds[3], (HEADS, SEQUENCE_ITEMS), jnp.float32, math.log(0.5), math.log(2.0)))
    shard_draw = jnp.exp(jax.random.uniform(stochastic_seeds[4], (HEADS, SEQUENCE_ITEMS // SEQ_ROWS), jnp.float32, math.log(0.5), math.log(2.0)))
    shard_multiplier = jnp.repeat(shard_draw, SEQ_ROWS, axis=1)
    spike_opening_slot = jax.random.randint(stochastic_seeds[5], (2, 1), 0, SEQUENCE_ITEMS)
    spike_span = jax.random.uniform(stochastic_seeds[6], (2, 1), jnp.float32, 0.22, 0.45)
    sequence_offsets = lax.broadcasted_iota(jnp.int32, (2, SEQUENCE_ITEMS), 1)
    spike_table = jnp.sum(jnp.where(sequence_offsets == spike_opening_slot, spike_span, 0.0), axis=0)
    return -(per_channel_forgetting * forgetting_noise * shard_multiplier) - spike_table[None, :]


def level_of(rng, dims, shards, low, largest):
    gain = 1.0
    for dim, parts in shards:
        steps = jax.random.uniform(jax.random.fold_in(jax.random.fold_in(rng, 6), dim), (parts,), jnp.float32, low / len(shards), largest / len(shards))
        gain = gain * jnp.repeat(jnp.exp(steps), dims[dim] // parts).reshape((-1,) + (1,) * (len(dims) - 1 - dim))
    return gain


def assign_block(key, own, number, rows, amount, top, limit, skew):
    ranking = jax.random.permutation(key, amount)
    heavy_load, usual = shares(amount, rows * top, limit, skew, True), shares(amount, rows * top, limit, skew, False)
    places = jnp.arange(amount)

    def named(lengths, turn):
        used = int((lengths > 0).sum())
        fixed = max(1, used // 4)
        passed = fixed + (places - fixed + turn * (used - fixed)) % max(1, amount - fixed)
        return jnp.zeros((amount,), jnp.int32).at[ranking[jnp.where(places < fixed, places, passed)]].set(jnp.asarray(lengths, jnp.int32))

    lengths = jnp.where(number % 4 == 0, named(heavy_load, number // 4), named(usual, number - number // 4 - 1))
    mixed = jax.random.permutation(jax.random.fold_in(own, 3), amount)
    giver, taker = mixed[0:amount // 2 * 2:2], mixed[1:amount // 2 * 2:2]
    room = jnp.minimum(lengths[giver] - 1, limit - lengths[taker]) // 2
    room = jnp.where((giver == ranking[0]) | (taker == ranking[0]) | (lengths[taker] == 0), 0, jnp.maximum(room, 0))
    passed = jax.random.randint(jax.random.fold_in(own, 4), (amount // 2,), 0, 1 << 20) % (room + 1)
    lengths = lengths.at[giver].add(-passed).at[taker].add(passed)
    members = jnp.searchsorted(jnp.cumsum(lengths), jnp.arange(rows * top), side="right").astype(jnp.int32)
    table = members.reshape(top, rows).T
    table = table[jax.random.permutation(jax.random.fold_in(own, 1), rows)]
    turn = jax.random.randint(jax.random.fold_in(own, 2), (rows, 1), 0, top)
    return jnp.take_along_axis(table, (jnp.arange(top)[None, :] + turn) % top, axis=1)


def shares(amount, total, limit, slope, full):
    portions = [(1 << 20) // math.isqrt(standing ** slope) + 1 for standing in range(1, amount + 1)]
    largest = limit if full else min(limit, max(-(-total // amount), total * portions[0] // sum(portions)))
    least = 1 if total - largest >= amount - 1 else 0
    given, spare = [largest] + [least] * (amount - 1), total - largest - least * (amount - 1)
    while spare > 0:
        free = [i for i in range(1, amount) if given[i] < largest] or [i for i in range(1, amount) if given[i] < limit]
        mass, remaining = sum([portions[i] for i in free]), spare
        for i in free:
            more = min(limit - given[i], max(1, remaining * portions[i] // mass), spare)
            given[i] = given[i] + more
            spare = spare - more
    return np.array(given)


def normal_values(key, dims, width, bound, cuts=(), kind=jnp.bfloat16):
    entries = width * jax.random.normal(key, dims, jnp.float32)
    if cuts:
        entries = entries * level_of(key, dims, cuts, -0.22, 0.18)
    return jnp.clip(entries, -bound, bound).astype(kind)


def setup_inputs(seed: int = 0) -> dict:
    streams_of = jax.random.split(jax.random.key(seed), 11)
    grad_out = normal_values(streams_of[0], (SEQUENCE_ITEMS, D), 1.0, 6.0, ((0, 256),))
    out_proj = normal_values(streams_of[1], (INNER, D), D ** -0.5, 0.125, ((0, 16),))
    step_size = jnp.clip(jnp.exp(math.log(0.1) - 4.6051702 * jax.random.uniform(streams_of[2], (HEADS, SEQUENCE_ITEMS), jnp.float32) ** level_of(streams_of[2], (HEADS, SEQUENCE_ITEMS), ((0, 16), (1, 16)), -0.2, 0.2)), 0.001, 0.1)
    log_decay = draw_log_decay(jax.random.fold_in(streams_of[10], 71), 0)
    b_input = normal_values(streams_of[4], (STATE, SEQUENCE_ITEMS), 0.25, 1.5, ((1, 16),), jnp.float32)
    c_output = normal_values(streams_of[5], (STATE, SEQUENCE_ITEMS), 0.25, 1.5, ((1, 16),), jnp.float32)
    skip_gain = jnp.clip(0.5 + 1.0 * jax.random.uniform(streams_of[6], (INNER,), jnp.float32) ** level_of(streams_of[6], (INNER,), ((0, 16),), -0.2, 0.2), 0.5, 1.5)
    expert_ids_keys = jax.random.split(jax.random.fold_in(streams_of[7], 1), SEQUENCE_ITEMS // TOK_DEV)
    expert_ids_turns = jax.random.permutation(jax.random.fold_in(streams_of[7], 3), SEQUENCE_ITEMS // TOK_DEV)
    expert_ids = jax.vmap(lambda own, number: assign_block(jax.random.fold_in(streams_of[7], 2), own, number, TOK_DEV, EXPERTS, TOP, CAP, 0))(expert_ids_keys, expert_ids_turns).reshape((SEQUENCE_ITEMS, TOP))
    hidden_act = normal_values(streams_of[8], (EXPERTS, SOURCES, CAP, FF), 1.0, 6.0, ((0, 16), (3, 16)))
    w_down = normal_values(streams_of[9], (EXPERTS, FF, D), (FF * D // 4) ** -0.5, 0.0029296875, ((0, 16), (1, 16)))
    return {"grad_out": grad_out, "out_proj": out_proj, "step_size": step_size, "log_decay": log_decay, "b_input": b_input, "c_output": c_output, "skip_gain": skip_gain, "expert_ids": expert_ids, "hidden_act": hidden_act, "w_down": w_down}


highest = lax.Precision.HIGHEST


def block_pass(state_in, pieces):
    grad_block, decay_block, step_block, b_block, c_block = pieces
    cum_decay = jnp.cumsum(decay_block, axis=1)
    gap_table = cum_decay[:, None, :] - cum_decay[:, :, None]
    upper_mask = lax.broadcasted_iota(jnp.int32, gap_table.shape, 2) >= lax.broadcasted_iota(jnp.int32, gap_table.shape, 1)
    weights = jnp.where(upper_mask, jnp.exp(jnp.where(upper_mask, gap_table, 0.0)), 0.0)
    intersection = lax.dot_general(b_block, c_block, (((0,), (0,)), ((), ())), precision=highest, preferred_element_type=jnp.float32)
    within = jnp.einsum("hut,thp->uhp", weights * intersection[None], grad_block, precision=highest)
    tail_decay = jnp.exp(cum_decay[:, -1:] - cum_decay)
    from_state = jnp.einsum("nu,hnp->uhp", b_block, state_in, precision=highest) * tail_decay.T[:, :, None]
    result = step_block.T[:, :, None] * (within + from_state)
    state_out = jnp.einsum("ht,nt,thp->hnp", jnp.exp(cum_decay), c_block, grad_block, precision=highest)
    state_out = state_out + jnp.exp(cum_decay[:, -1])[:, None, None] * state_in
    return state_out, result


def local_sweep(grad_rows, decay_rows, step_rows, b_rows, c_rows, start_state):
    row_count = grad_rows.shape[0]
    head_count = decay_rows.shape[0]
    block_len = min(512, row_count)
    block_count = row_count // block_len
    pieces = (grad_rows.reshape(block_count, block_len, head_count, grad_rows.shape[2]),
              decay_rows.reshape(head_count, block_count, block_len).transpose(1, 0, 2),
              step_rows.reshape(head_count, block_count, block_len).transpose(1, 0, 2),
              b_rows.reshape(b_rows.shape[0], block_count, block_len).transpose(1, 0, 2),
              c_rows.reshape(c_rows.shape[0], block_count, block_len).transpose(1, 0, 2))
    state_out, results = lax.scan(block_pass, start_state, pieces, reverse=True)
    return state_out, results.reshape(row_count, head_count, grad_rows.shape[2])


def route_table(groups, expert, cap_len):
    hit_mask = jnp.any(groups == expert, axis=2)
    rank_ids = jnp.cumsum(hit_mask.astype(jnp.int32), axis=1) - 1
    slot_ids = lax.broadcasted_iota(jnp.int32, (1, 1, cap_len), 2)
    chosen = jnp.logical_and(hit_mask[:, :, None], rank_ids[:, :, None] == slot_ids)
    token_ids = lax.broadcasted_iota(jnp.int32, chosen.shape, 1)
    position = jnp.sum(jnp.where(chosen, token_ids, 0), axis=1).astype(jnp.int32)
    filled = jnp.any(chosen, axis=1)
    return position, filled


def slot_lookup(slot_table, own_ids, cap_len, expert_count):
    experts_iota = lax.broadcasted_iota(jnp.int32, (1, 1, expert_count), 2)
    onehot = own_ids[:, :, None] == experts_iota
    member = jnp.any(onehot, axis=1).astype(jnp.int32)
    rank_ids = jnp.cumsum(member, axis=0) - 1
    slot_of = jnp.sum(jnp.where(onehot, rank_ids[:, None, :], 0), axis=2)
    picked = jnp.sum(jnp.where(onehot[:, :, :, None], slot_table[None, None], 0.0), axis=2)
    slot_iota = lax.broadcasted_iota(jnp.int32, (1, 1, cap_len), 2)
    return jnp.sum(jnp.where(slot_of[:, :, None] == slot_iota, picked, 0.0), axis=2)


def reference(grad_out, out_proj, step_size, log_decay, b_input, c_output, skip_gain, expert_ids, hidden_act, w_down):
    inner_grad = jnp.dot(grad_out, out_proj.T, preferred_element_type=jnp.float32)
    start_state = jnp.zeros((HEADS, STATE, HEAD), jnp.float32)
    unused, swept_part = local_sweep(inner_grad.reshape(SEQUENCE_ITEMS, HEADS, HEAD), log_decay, step_size, b_input, c_output, start_state)
    d_inner = (swept_part.reshape(SEQUENCE_ITEMS, INNER) + skip_gain * inner_grad).astype(jnp.bfloat16)
    groups = expert_ids.reshape(SOURCES, TOK_DEV, TOP)
    sources = grad_out.reshape(SOURCES, TOK_DEV, D)

    def per_expert(pieces):
        expert, saved_part, weights = pieces
        position, filled = route_table(groups, expert, CAP)
        slot_rows = jnp.take_along_axis(sources, position[:, :, None], axis=1)
        slot_rows = jnp.where(filled[:, :, None], slot_rows, jnp.zeros_like(slot_rows))
        projected = jnp.dot(slot_rows.reshape(SOURCES * CAP, D), weights.T, preferred_element_type=jnp.float32)
        scores = jnp.sum(projected * saved_part.reshape(SOURCES * CAP, FF).astype(jnp.float32), axis=1)
        return scores.reshape(SOURCES, CAP)

    slot_scores = lax.map(per_expert, (jnp.arange(EXPERTS, dtype=jnp.int32), hidden_act, w_down))
    lookup = partial(slot_lookup, cap_len=CAP, expert_count=EXPERTS)
    values = jax.vmap(lookup, in_axes=(1, 0))(slot_scores, groups)
    d_gate = values.reshape(SEQUENCE_ITEMS, TOP).T
    return d_inner, d_gate
```

```python
import functools

import jax
import jax.numpy as jnp
from jax import lax
from jax.experimental import pallas as pl
from jax.experimental.pallas import tpu as pltpu
from jax.sharding import PartitionSpec as P

HEAD = 64
MESH = pl.DeviceIdType.MESH
F32, BF16 = jnp.float32, jnp.bfloat16

CAP = 18
HALF = (16, 32, 32, 32, 32)
OFF = (0, 16, 48, 80, 112)
BASE = (0, 256, 768, 1280, 1792)
RANK = (0, -1, 1, -2, 2, -3, 3, 4)
VMEM_ANY = pl.BlockSpec(memory_space=pltpu.VMEM)
HBM_ANY = pl.BlockSpec(memory_space=pl.ANY)


def dot_t(a, b):
    return lax.dot_general(a, b, (((1,), (1,)), ((), ())), preferred_element_type=F32)


def dot_n(a, b):
    return lax.dot_general(a, b, (((1,), (0,)), ((), ())), preferred_element_type=F32)


def dot_tn(a, b):
    return lax.dot_general(a, b, (((0,), (0,)), ((), ())), preferred_element_type=F32)


def halves(x):
    hi = x.astype(BF16)
    return hi, (x - hi.astype(F32)).astype(BF16)


def order_matrix(z, yl):
    row = lax.broadcasted_iota(jnp.int32, (288, 288), 0)
    col = lax.broadcasted_iota(jnp.int32, (288, 288), 1)
    late = row - 32
    side = jnp.where(row < 32, row >> 4, (late >> 5) & 1)
    place = jnp.where(row < 32, row & 15, 16 + ((late >> 6) << 5) + (late & 31))
    arrival = (place * 3641) >> 16
    slot = place - 18 * arrival
    shift = jnp.where((arrival & 1) == 1, -((arrival + 1) >> 1), arrival >> 1)
    source = (z + shift) & 7
    lane = jnp.where(side == 0, yl, 1 - yl)
    return col == slot * 16 + lane * 8 + source


def comm_kernel(
    g_hbm, w_hbm, ids, hid, wd_hbm, inner, scores,
    blocks, proj, outbox, rows, picks, wd, act, acts, keys, send, recv, local,
):
    s, e = lax.axis_index("seq"), lax.axis_index("exp")
    core, x, yh = s % 2, (s // 2) % 4, s // 8
    z, yl = e % 8, e // 8
    mine, other = yh * 4 + x, (1 - yh) * 4 + x
    plane = lambda yh_, x_: (yh_ * 4 + x_) * 2 + core
    zp, zm = (s, yl * 8 + (z + 1) % 8), (s, yl * 8 + (z + 7) % 8)
    xp, xm = (plane(yh, (x + 1) % 4), e), (plane(yh, (x + 3) % 4), e)
    yp, yq = (s, (1 - yl) * 8 + z), (plane(1 - yh, x), e)
    yd = (plane(1 - yh, x), (1 - yl) * 8 + z)
    sib = ((yh * 4 + x) * 2 + 1 - core, e)
    peers = (zp, zm, xp, xm, yp, yq, yd, sib)
    names, pending = {}, []

    def start(name, src, dst, to):
        i = names.setdefault(name, len(names))
        copy = pltpu.make_async_remote_copy(
            src_ref=src, dst_ref=dst, send_sem=send.at[i], recv_sem=recv.at[i],
            device_id=to, device_id_type=MESH,
        )
        copy.start()
        pending.append(copy)

    def arrived(name, dst):
        i = names[name]
        pltpu.make_async_remote_copy(
            src_ref=dst, dst_ref=dst, send_sem=send.at[i], recv_sem=recv.at[i],
            device_id=sib, device_id_type=MESH,
        ).wait_recv()

    def part(k, j, side=None):
        h = HALF[k]
        at = pl.multiple_of(BASE[k] + j * (2 * h), 2 * h)
        if side is None:
            return rows.at[pl.ds(at, 2 * h)]
        return rows.at[pl.ds(pl.multiple_of(at + side * h, 16), h)]

    spot = lambda a: (z + RANK[a] + 8) % 8
    loads = [
        pltpu.make_async_copy(g_hbm, blocks.at[z], local.at[0]),
        pltpu.make_async_copy(w_hbm, proj.at[yl], local.at[1]),
        pltpu.make_async_copy(wd_hbm, wd.at[core], local.at[2]),
        pltpu.make_async_copy(hid.at[:, :, core], act.at[core], local.at[3]),
    ]
    for load in loads:
        load.start()
    barrier = pltpu.get_barrier_semaphore()
    for peer in peers:
        pl.semaphore_signal(barrier, inc=1, device_id=peer, device_id_type=MESH)
    pl.semaphore_wait(barrier, len(peers))

    loads[0].wait()
    start("zp0", blocks.at[z], blocks.at[z], zp)
    start("zm0", blocks.at[z], blocks.at[z], zm)
    part_of_w = pl.ds(pl.multiple_of(core * 128, 128), 128)
    rest_of_w = pl.ds(pl.multiple_of((1 - core) * 128, 128), 128)
    loads[1].wait()
    start("w", proj.at[yl, part_of_w], proj.at[yl, part_of_w], yp)
    start("wd", wd_hbm, wd.at[core], sib)
    start("hid", hid.at[:, :, 1 - core], act.at[core], sib)

    for a in range(8):
        lanes = pl.ds(pl.multiple_of((yl * 8 + spot(a)) * 128, 128), 128)
        named = ids[:, lanes]
        for side, expert in ((0, e), (1, (1 - yl) * 8 + z)):
            hit = (named[0:1] == expert) | (named[1:2] == expert)
            keys[2 * a + side : 2 * a + side + 1, :] = jnp.where(hit, 1.0, 0.0)
    hits = keys[...]
    tri = lax.broadcasted_iota(jnp.int32, (128, 128), 0) <= lax.broadcasted_iota(
        jnp.int32, (128, 128), 1
    )
    rank = dot_n(hits.astype(BF16), jnp.where(tri, 1.0, 0.0).astype(BF16))
    keys[...] = jnp.where(hits > 0.5, rank - 1.0, -1000.0)

    def pick(k):
        h = HALF[k]
        place = lax.broadcasted_iota(jnp.int32, (h, 128), 0) + OFF[k]
        first, last = OFF[k] // CAP, (OFF[k] + h - 1) // CAP
        wanted = []
        for a in range(first, last + 1):
            at = (place - CAP * a).astype(F32)
            sides = [keys[2 * a + side : 2 * a + side + 1, :] == at for side in (0, 1)]
            wanted.append(
                jnp.concatenate([jnp.where(m, 1.0, 0.0) for m in sides], axis=0).astype(BF16)
            )
        for n in range(0, 2048, 512):
            found = None
            for a, chosen in zip(range(first, last + 1), wanted):
                more = dot_n(chosen, blocks[spot(a), :, n : n + 512])
                found = more if found is None else found + more
            found = found.astype(BF16)
            at = pl.multiple_of(BASE[k] + mine * (2 * h), 2 * h)
            rows[pl.ds(at, h), n : n + 512] = found[:h]
            picks[OFF[k] : OFF[k] + h, n : n + 512] = found[h:]

    def pick_and_send(k):
        pick(k)
        cut = picks.at[OFF[k] : OFF[k] + HALF[k]]
        start(f"pl{k}", cut, part(k, mine, 1), yp)
        start(f"pd{k}", cut, part(k, mine, 1), yd)
        start(f"ow{k}", part(k, mine, 0), part(k, mine, 0), yq)

    def spread(k):
        arrived(f"pl{k}", part(k, mine, 1))
        start(f"xpa{k}", part(k, mine), part(k, mine), xp)
        start(f"xma{k}", part(k, mine), part(k, mine), xm)
        arrived(f"pd{k}", part(k, other, 1))
        arrived(f"ow{k}", part(k, other, 0))
        start(f"xpb{k}", part(k, other), part(k, other), xp)
        start(f"xmb{k}", part(k, other), part(k, other), xm)

    def relay(k):
        for tag, side in (("a", yh), ("b", 1 - yh)):
            before, after = side * 4 + (x + 3) % 4, side * 4 + (x + 1) % 4
            arrived(f"xp{tag}{k}", part(k, before))
            start(f"fp{tag}{k}", part(k, before, 0), part(k, before, 0), xp)
            arrived(f"xm{tag}{k}", part(k, after))
            start(f"fm{tag}{k}", part(k, after, 1), part(k, after, 1), xm)

    def relayed(k):
        for tag, side in (("a", yh), ("b", 1 - yh)):
            far = side * 4 + (x + 2) % 4
            arrived(f"fp{tag}{k}", part(k, far, 0))
            arrived(f"fm{tag}{k}", part(k, far, 1))

    def ring(k):
        back, ahead = (z - k + 8) % 8, (z + k) % 8
        if k < 4:
            arrived(f"zp{k - 1}", blocks.at[back])
            arrived(f"zm{k - 1}", blocks.at[ahead])
        else:
            arrived("zp3", blocks.at[back, 0:64])
            arrived("zm3", blocks.at[ahead, 64:128])
        if k < 3:
            start(f"zp{k}", blocks.at[back], blocks.at[back], zp)
            start(f"zm{k}", blocks.at[ahead], blocks.at[ahead], zm)
        elif k == 3:
            start("zp3", blocks.at[back, 0:64], blocks.at[back, 0:64], zp)
            start("zm3", blocks.at[ahead, 64:128], blocks.at[ahead, 64:128], zm)

    def product(a):
        block = blocks[spot(a)]
        outbox[a] = dot_t(block, proj[1 - yl])
        to = pl.ds(pl.multiple_of((yl * 8 + spot(a)) * 128, 128), 128)
        start(f"c{a}", outbox.at[a], inner.at[to], yp)
        inner[to, :] = dot_t(block, proj[yl])

    def ordered():
        loads[3].wait()
        arrived("hid", act.at[1 - core])
        matrix = jnp.where(order_matrix(z, yl), 1.0, 0.0).astype(BF16)

        def step(i, _):
            j, c = i // 2, i % 2
            source = act[c, :, j].reshape(288, 512)
            put = dot_n(matrix, source).astype(BF16)
            for k in range(5):
                h = HALF[k]
                at = pl.multiple_of(BASE[k] + j * (2 * h), 2 * h)
                acts[c, pl.ds(at, 2 * h), :] = put[2 * OFF[k] : 2 * OFF[k] + 2 * h]
            return 0

        lax.fori_loop(0, 16, step, 0)

    def score(m):
        at = pl.multiple_of(m * 256, 256)
        lhs = rows[pl.ds(at, 256), :]

        def step(i, total):
            c, n = i // 2, pl.multiple_of((i % 2) * 256, 256)
            got = dot_t(lhs, wd[c, pl.ds(n, 256), :])
            prod = got * acts[c, pl.ds(at, 256), pl.ds(n, 256)].astype(F32)
            return total + prod[:, :128] + prod[:, 128:]

        total = lax.fori_loop(0, 4, step, jnp.zeros((256, 128), F32))
        scores[pl.ds(m, 1), :] = jnp.sum(total.T, axis=0, keepdims=True)

    pick_and_send(0)
    spread(0)
    ring(1)
    pick_and_send(1)
    arrived("w", proj.at[1 - yl, part_of_w])
    start("wf", proj.at[1 - yl, part_of_w], proj.at[1 - yl, part_of_w], sib)
    ordered()
    spread(1)
    ring(2)
    pick_and_send(2)
    arrived("wf", proj.at[1 - yl, rest_of_w])
    for a in range(3):
        product(a)
    spread(2)
    relay(0)
    ring(3)
    pick_and_send(3)
    for a in range(3, 5):
        product(a)
    spread(3)
    relay(1)
    ring(4)
    pick_and_send(4)
    for a in range(5, 8):
        product(a)
    spread(4)
    relay(2)
    for a in range(8):
        to = pl.ds(pl.multiple_of(((1 - yl) * 8 + spot(a)) * 128, 128), 128)
        arrived(f"c{a}", inner.at[to])
    loads[2].wait()
    arrived("wd", wd.at[1 - core])
    relayed(0)
    score(0)
    relay(3)
    relayed(1)
    lax.fori_loop(1, 3, lambda m, _: (score(m), 0)[1], 0)
    relay(4)
    for k in range(2, 5):
        relayed(k)
        lax.fori_loop(2 * k - 1, 2 * k + 1, lambda m, _: (score(m), 0)[1], 0)
    for copy in pending:
        copy.wait_send()


def chunk_decays(ld, cum, cum_t):
    lines = [
        jnp.concatenate([ld[:, 128 * i : 128 * (i + 1)], jnp.zeros((4, 128), F32)], axis=0)
        for i in range(16)
    ]
    x = jnp.concatenate(lines, axis=0)
    hi, rest = x.astype(BF16), None
    rest = x - hi.astype(F32)
    mid, low = halves(rest)
    tri = lax.broadcasted_iota(jnp.int32, (128, 128), 0) <= lax.broadcasted_iota(
        jnp.int32, (128, 128), 1
    )
    tri = jnp.where(tri, 1.0, 0.0).astype(BF16)
    total = (dot_n(low, tri) + dot_n(mid, tri)) + dot_n(hi, tri)
    for i in range(16):
        cum[i] = total[8 * i : 8 * i + 8]
    if cum_t is not None:
        turned = total.T
        for i in range(16):
            cum_t[i] = turned[:, 8 * i : 8 * i + 8]


def by_head(values):
    lane = lax.broadcasted_iota(jnp.int32, (1, 256), 1) // HEAD
    out = jnp.broadcast_to(values[3], (1, 256))
    for i in (2, 1, 0):
        out = jnp.where(lane == i, jnp.broadcast_to(values[i], (1, 256)), out)
    return out


def chunk_state(inner, c_in, cum, i):
    at = pl.ds(pl.multiple_of(i * 128, 128), 128)
    grown = jnp.exp(cum[i])
    c = c_in[:, at]
    hi, low = halves(jnp.concatenate([c * grown[h : h + 1] for h in range(4)], axis=0))
    g_hi, g_low = halves(inner[at, :])
    left = jnp.concatenate([hi, low, hi], axis=1)
    right = jnp.concatenate([g_hi, g_hi, g_low], axis=0)
    full = dot_n(left, right)
    lane = lax.broadcasted_iota(jnp.int32, (16, 256), 1) // HEAD
    out = full[48:64]
    for h in (2, 1, 0):
        out = jnp.where(lane == h, full[16 * h : 16 * h + 16], out)
    return out


def chunk_total(cum, i):
    ends = cum[i]
    return by_head([ends[h : h + 1, 127:128] for h in range(4)])


def summary_kernel(inner, ld, c_in, out, cum):
    chunk_decays(ld, cum, None)

    def step(n, carry):
        state, total = carry
        i = 15 - n
        ends = chunk_total(cum, i)
        return chunk_state(inner, c_in, cum, i) + jnp.exp(ends) * state, total + ends

    state, total = lax.fori_loop(
        0, 16, step, (jnp.zeros((16, 256), F32), jnp.zeros((1, 256), F32)), unroll=2
    )
    out[0:16] = state
    out[16:24] = jnp.broadcast_to(total, (8, 256))


def sweep_kernel(inner, ld, st, b_in, c_in, gain, states, out, cum, cum_t, step_t):
    me = lax.axis_index("seq")
    chunk_decays(ld, cum, cum_t)
    lines = [
        jnp.concatenate([st[:, 128 * i : 128 * (i + 1)], jnp.zeros((4, 128), F32)], axis=0)
        for i in range(16)
    ]
    turned = jnp.concatenate(lines, axis=0).T
    for i in range(16):
        step_t[i] = turned[:, 8 * i : 8 * i + 8]

    def enter(n, state):
        k = 15 - n
        got = states[k]
        return jnp.where(k > me, got[0:16] + jnp.exp(got[16:17]) * state, state)

    state = lax.fori_loop(0, 16, enter, jnp.zeros((16, 256), F32))
    upper = lax.broadcasted_iota(jnp.int32, (128, 128), 1) >= lax.broadcasted_iota(
        jnp.int32, (128, 128), 0
    )
    left_lanes = lax.broadcasted_iota(jnp.int32, (128, 128), 1) < HEAD
    gains = gain[...]

    def step(n, state):
        i = 15 - n
        at = pl.ds(pl.multiple_of(i * 128, 128), 128)
        b_hi, b_low = halves(b_in[:, at])
        c_hi, c_low = halves(c_in[:, at])
        b_all = jnp.concatenate([b_hi, b_low, b_hi], axis=0)
        table = dot_tn(b_all, jnp.concatenate([c_hi, c_hi, c_low], axis=0))
        s_hi, s_low = halves(state)
        carried = dot_tn(b_all, jnp.concatenate([s_hi, s_hi, s_low], axis=0))
        rows_, cols, steps = cum[i], cum_t[i], step_t[i]
        for p in (0, 1):
            lanes = slice(128 * p, 128 * p + 128)
            g = inner[at, lanes]
            tail, size = [], []
            m_hi, m_low = [], []
            for h in (2 * p, 2 * p + 1):
                col = jnp.broadcast_to(cols[:, h : h + 1], (128, 128))
                row = rows_[h : h + 1]
                gap = jnp.where(upper, row - col, 0.0)
                weight = jnp.where(upper, jnp.exp(gap), 0.0) * table
                hi, low = halves(weight)
                m_hi.append(hi)
                m_low.append(low)
                tail.append(jnp.exp(row[:, 127:128] - col))
                size.append(jnp.broadcast_to(steps[:, h : h + 1], (128, 128)))
            g_a, g_b = halves(jnp.where(left_lanes, g, 0.0)), halves(jnp.where(left_lanes, 0.0, g))
            left = jnp.concatenate(m_hi + m_low + m_hi, axis=1)
            right = jnp.concatenate([g_a[0], g_b[0], g_a[0], g_b[0], g_a[1], g_b[1]], axis=0)
            within = dot_n(left, right)
            tails = jnp.where(left_lanes, tail[0], tail[1])
            sizes = jnp.where(left_lanes, size[0], size[1])
            value = sizes * (within + carried[:, lanes] * tails) + gains[:, lanes] * g
            out[at, lanes] = value.astype(BF16)
        return chunk_state(inner, c_in, cum, i) + jnp.exp(chunk_total(cum, i)) * state

    lax.fori_loop(0, 16, step, state)


def slot_lookup(slot_table, own_ids, cap_len, expert_count):
    experts_iota = lax.broadcasted_iota(jnp.int32, (1, 1, expert_count), 2)
    onehot = own_ids[:, :, None] == experts_iota
    member = jnp.any(onehot, axis=1).astype(jnp.int32)
    rank_ids = jnp.cumsum(member, axis=0) - 1
    slot_of = jnp.sum(jnp.where(onehot, rank_ids[:, None, :], 0), axis=2)
    picked = jnp.sum(jnp.where(onehot[:, :, :, None], slot_table[None, None], 0.0), axis=2)
    slot_iota = lax.broadcasted_iota(jnp.int32, (1, 1, cap_len), 2)
    return jnp.sum(jnp.where(slot_of[:, :, None] == slot_iota, picked, 0.0), axis=2)


def shards(
    grad_out, out_proj, step_size, log_decay, b_input, c_output,
    skip_gain, expert_ids, hidden_act, w_down,
):
    s, e = lax.axis_index("seq"), lax.axis_index("exp")
    big = pltpu.CompilerParams(vmem_limit_bytes=60 * 1024 * 1024)
    hidden = hidden_act[0].transpose(1, 0, 2).reshape(18, 8, 2, 16, 512)
    inner, scores = pl.pallas_call(
        comm_kernel,
        name="gather_and_score",
        out_shape=(
            jax.ShapeDtypeStruct((2048, 256), F32),
            jax.ShapeDtypeStruct((9, 256), F32),
        ),
        in_specs=[HBM_ANY, HBM_ANY, VMEM_ANY, HBM_ANY, HBM_ANY],
        out_specs=(VMEM_ANY, VMEM_ANY),
        scratch_shapes=[
            pltpu.VMEM((8, 128, 2048), BF16),
            pltpu.VMEM((2, 256, 2048), BF16),
            pltpu.VMEM((8, 128, 256), F32),
            pltpu.VMEM((2304, 2048), BF16),
            pltpu.VMEM((144, 2048), BF16),
            pltpu.VMEM((2, 512, 2048), BF16),
            pltpu.VMEM((2, 18, 8, 16, 512), BF16),
            pltpu.VMEM((2, 2304, 512), BF16),
            pltpu.VMEM((16, 128), F32),
            pltpu.SemaphoreType.DMA((80,)),
            pltpu.SemaphoreType.DMA((80,)),
            pltpu.SemaphoreType.DMA((4,)),
        ],
        compiler_params=pltpu.CompilerParams(
            collective_id=0, has_side_effects=True, vmem_limit_bytes=60 * 1024 * 1024
        ),
    )(grad_out, out_proj, expert_ids.T, hidden, w_down[0])

    payload = pl.pallas_call(
        summary_kernel,
        name="summary",
        out_shape=jax.ShapeDtypeStruct((24, 256), F32),
        in_specs=[VMEM_ANY] * 3,
        out_specs=VMEM_ANY,
        scratch_shapes=[pltpu.VMEM((16, 8, 128), F32)],
        compiler_params=big,
    )(inner, log_decay, c_output)
    states = lax.all_to_all(
        jnp.broadcast_to(payload, (16, 24, 256)), "seq", split_axis=0, concat_axis=0, tiled=True
    )
    d_inner = pl.pallas_call(
        sweep_kernel,
        name="sweep",
        out_shape=jax.ShapeDtypeStruct((2048, 256), BF16),
        in_specs=[VMEM_ANY] * 7,
        out_specs=VMEM_ANY,
        scratch_shapes=[
            pltpu.VMEM((16, 8, 128), F32),
            pltpu.VMEM((16, 128, 8), F32),
            pltpu.VMEM((16, 128, 8), F32),
        ],
        compiler_params=big,
    )(inner, log_decay, step_size, b_input, c_output, skip_gain.reshape(1, 256), states)

    flat = scores.reshape(2304)
    late = flat[256:].reshape(4, 8, 64).transpose(1, 0, 2).reshape(8, 256)
    placed = jnp.concatenate([flat[:256].reshape(8, 32), late], axis=1)
    matrix = jnp.where(order_matrix(e % 8, e // 8), 1.0, 0.0)
    natural = jnp.dot(placed, matrix, precision=lax.Precision.HIGHEST)
    both = jnp.where((jnp.arange(2) == s % 2)[None, :, None], natural[:, None, :], 0.0)
    parts = lax.all_to_all(both.reshape(16, 288), "seq", 0, 0, tiled=True)
    summed = jnp.sum(parts, axis=0).reshape(18, 16).T
    slot_table = lax.all_to_all(
        summed.reshape(16, 1, 18), "exp", split_axis=0, concat_axis=1, tiled=True
    ).reshape(16, 18)
    own_ids = lax.dynamic_slice_in_dim(expert_ids, e * 128, 128, 0)
    d_gate = slot_lookup(slot_table, own_ids, 18, 16).T
    return d_inner, d_gate


def solution(mesh):
    in_specs = (
        P(("seq", "exp"), None),
        P("exp", None),
        P("exp", "seq"),
        P("exp", "seq"),
        P(None, "seq"),
        P(None, "seq"),
        P("exp"),
        P("seq", None),
        P("exp", None, None, "seq"),
        P("exp", "seq", None),
    )
    out_specs = (P("seq", "exp"), P(None, ("seq", "exp")))
    return jax.shard_map(shards, mesh=mesh, in_specs=in_specs, out_specs=out_specs, check_vma=False)
```

```python
import jax
import jax.numpy as jnp
from jax import lax
from jax.experimental import pallas as pl
from jax.experimental.pallas import tpu as pltpu
from jax.sharding import PartitionSpec as P

HEAD = 64
MESH = pl.DeviceIdType.MESH
F32, BF16 = jnp.float32, jnp.bfloat16

CAP = 18
HALF = (16, 32, 32, 32, 32)
OFF = (0, 16, 48, 80, 112)
BASE = (0, 256, 768, 1280, 1792)
RANK = (0, -1, 1, -2, 2, -3, 3, 4)
VMEM_ANY = pl.BlockSpec(memory_space=pltpu.VMEM)
HBM_ANY = pl.BlockSpec(memory_space=pl.ANY)


def dot_t(a, b):
    return lax.dot_general(a, b, (((1,), (1,)), ((), ())), preferred_element_type=F32)


def dot_n(a, b):
    return lax.dot_general(a, b, (((1,), (0,)), ((), ())), preferred_element_type=F32)


def dot_tn(a, b):
    return lax.dot_general(a, b, (((0,), (0,)), ((), ())), preferred_element_type=F32)


def halves(x):
    hi = x.astype(BF16)
    return hi, (x - hi.astype(F32)).astype(BF16)


def order_matrix(z, yl):
    row = lax.broadcasted_iota(jnp.int32, (288, 288), 0)
    col = lax.broadcasted_iota(jnp.int32, (288, 288), 1)
    late = row - 32
    side = jnp.where(row < 32, row >> 4, (late >> 5) & 1)
    place = jnp.where(row < 32, row & 15, 16 + ((late >> 6) << 5) + (late & 31))
    arrival = (place * 3641) >> 16
    slot = place - 18 * arrival
    shift = jnp.where((arrival & 1) == 1, -((arrival + 1) >> 1), arrival >> 1)
    source = (z + shift) & 7
    lane = jnp.where(side == 0, yl, 1 - yl)
    return col == slot * 16 + lane * 8 + source


def comm_kernel(
    g_hbm, w_hbm, ids, hid, wd_hbm, ld, st, b_in, c_in, gain, out, gate,
    inner, blocks, proj, outbox, rows, picks, wd, act, acts, keys, scores, sent, parts, tables,
    cum, cum_t, step_t, pair, chips, send, recv, local,
):
    s, e = lax.axis_index("seq"), lax.axis_index("exp")
    core, x, yh = s % 2, (s // 2) % 4, s // 8
    z, yl = e % 8, e // 8
    mine, other = yh * 4 + x, (1 - yh) * 4 + x
    plane = lambda yh_, x_: (yh_ * 4 + x_) * 2 + core
    zp, zm = (s, yl * 8 + (z + 1) % 8), (s, yl * 8 + (z + 7) % 8)
    xp, xm = (plane(yh, (x + 1) % 4), e), (plane(yh, (x + 3) % 4), e)
    yp, yq = (s, (1 - yl) * 8 + z), (plane(1 - yh, x), e)
    yd = (plane(1 - yh, x), (1 - yl) * 8 + z)
    sib = ((yh * 4 + x) * 2 + 1 - core, e)
    peers = (zp, zm, xp, xm, yp, yq, yd, sib)
    names, pending = {}, []

    def start(name, src, dst, to):
        i = names.setdefault(name, len(names))
        copy = pltpu.make_async_remote_copy(
            src_ref=src, dst_ref=dst, send_sem=send.at[i], recv_sem=recv.at[i],
            device_id=to, device_id_type=MESH,
        )
        copy.start()
        pending.append(copy)

    def arrived(name, dst):
        i = names[name]
        pltpu.make_async_remote_copy(
            src_ref=dst, dst_ref=dst, send_sem=send.at[i], recv_sem=recv.at[i],
            device_id=sib, device_id_type=MESH,
        ).wait_recv()

    def part(k, j, side=None):
        h = HALF[k]
        at = pl.multiple_of(BASE[k] + j * (2 * h), 2 * h)
        if side is None:
            return rows.at[pl.ds(at, 2 * h)]
        return rows.at[pl.ds(pl.multiple_of(at + side * h, 16), h)]

    spot = lambda a: (z + RANK[a] + 8) % 8
    loads = [
        pltpu.make_async_copy(g_hbm, blocks.at[z], local.at[0]),
        pltpu.make_async_copy(w_hbm, proj.at[yl], local.at[1]),
        pltpu.make_async_copy(wd_hbm, wd.at[core], local.at[2]),
        pltpu.make_async_copy(hid.at[:, :, core], act.at[core], local.at[3]),
    ]
    for load in loads:
        load.start()
    barrier = pltpu.get_barrier_semaphore()
    for peer in peers:
        pl.semaphore_signal(barrier, inc=1, device_id=peer, device_id_type=MESH)
    pl.semaphore_wait(barrier, len(peers))

    loads[0].wait()
    start("zp0", blocks.at[z], blocks.at[z], zp)
    start("zm0", blocks.at[z], blocks.at[z], zm)
    part_of_w = pl.ds(pl.multiple_of(core * 128, 128), 128)
    rest_of_w = pl.ds(pl.multiple_of((1 - core) * 128, 128), 128)
    loads[1].wait()
    start("w", proj.at[yl, part_of_w], proj.at[yl, part_of_w], yp)
    start("wd", wd_hbm, wd.at[core], sib)
    start("hid", hid.at[:, :, 1 - core], act.at[core], sib)

    for a in range(8):
        lanes = pl.ds(pl.multiple_of((yl * 8 + spot(a)) * 128, 128), 128)
        named = ids[:, lanes]
        for side, expert in ((0, e), (1, (1 - yl) * 8 + z)):
            hit = (named[0:1] == expert) | (named[1:2] == expert)
            keys[2 * a + side : 2 * a + side + 1, :] = jnp.where(hit, 1.0, 0.0)
    hits = keys[...]
    tri = lax.broadcasted_iota(jnp.int32, (128, 128), 0) <= lax.broadcasted_iota(
        jnp.int32, (128, 128), 1
    )
    rank = dot_n(hits.astype(BF16), jnp.where(tri, 1.0, 0.0).astype(BF16))
    keys[...] = jnp.where(hits > 0.5, rank - 1.0, -1000.0)

    def pick(k):
        h = HALF[k]
        place = lax.broadcasted_iota(jnp.int32, (h, 128), 0) + OFF[k]
        first, last = OFF[k] // CAP, (OFF[k] + h - 1) // CAP
        wanted = []
        for a in range(first, last + 1):
            at = (place - CAP * a).astype(F32)
            sides = [keys[2 * a + side : 2 * a + side + 1, :] == at for side in (0, 1)]
            wanted.append(
                jnp.concatenate([jnp.where(m, 1.0, 0.0) for m in sides], axis=0).astype(BF16)
            )
        for n in range(0, 2048, 512):
            found = None
            for a, chosen in zip(range(first, last + 1), wanted):
                more = dot_n(chosen, blocks[spot(a), :, n : n + 512])
                found = more if found is None else found + more
            found = found.astype(BF16)
            at = pl.multiple_of(BASE[k] + mine * (2 * h), 2 * h)
            rows[pl.ds(at, h), n : n + 512] = found[:h]
            picks[OFF[k] : OFF[k] + h, n : n + 512] = found[h:]

    def pick_and_send(k):
        pick(k)
        cut = picks.at[OFF[k] : OFF[k] + HALF[k]]
        start(f"pl{k}", cut, part(k, mine, 1), yp)
        start(f"pd{k}", cut, part(k, mine, 1), yd)
        start(f"ow{k}", part(k, mine, 0), part(k, mine, 0), yq)

    def spread(k):
        arrived(f"pl{k}", part(k, mine, 1))
        start(f"xpa{k}", part(k, mine), part(k, mine), xp)
        start(f"xma{k}", part(k, mine), part(k, mine), xm)
        arrived(f"pd{k}", part(k, other, 1))
        arrived(f"ow{k}", part(k, other, 0))
        start(f"xpb{k}", part(k, other), part(k, other), xp)
        start(f"xmb{k}", part(k, other), part(k, other), xm)

    def relay(k):
        for tag, side in (("a", yh), ("b", 1 - yh)):
            before, after = side * 4 + (x + 3) % 4, side * 4 + (x + 1) % 4
            arrived(f"xp{tag}{k}", part(k, before))
            start(f"fp{tag}{k}", part(k, before, 0), part(k, before, 0), xp)
            arrived(f"xm{tag}{k}", part(k, after))
            start(f"fm{tag}{k}", part(k, after, 1), part(k, after, 1), xm)

    def relayed(k):
        for tag, side in (("a", yh), ("b", 1 - yh)):
            far = side * 4 + (x + 2) % 4
            arrived(f"fp{tag}{k}", part(k, far, 0))
            arrived(f"fm{tag}{k}", part(k, far, 1))

    def ring(k):
        back, ahead = (z - k + 8) % 8, (z + k) % 8
        if k < 4:
            arrived(f"zp{k - 1}", blocks.at[back])
            arrived(f"zm{k - 1}", blocks.at[ahead])
        else:
            arrived("zp3", blocks.at[back, 0:64])
            arrived("zm3", blocks.at[ahead, 64:128])
        if k < 3:
            start(f"zp{k}", blocks.at[back], blocks.at[back], zp)
            start(f"zm{k}", blocks.at[ahead], blocks.at[ahead], zm)
        elif k == 3:
            start("zp3", blocks.at[back, 0:64], blocks.at[back, 0:64], zp)
            start("zm3", blocks.at[ahead, 64:128], blocks.at[ahead, 64:128], zm)

    def product(a):
        block = blocks[spot(a)]
        outbox[a] = dot_t(block, proj[1 - yl])
        to = pl.ds(pl.multiple_of((yl * 8 + spot(a)) * 128, 128), 128)
        start(f"c{a}", outbox.at[a], inner.at[to], yp)
        inner[to, :] = dot_t(block, proj[yl])

    def ordered():
        loads[3].wait()
        arrived("hid", act.at[1 - core])
        matrix = jnp.where(order_matrix(z, yl), 1.0, 0.0).astype(BF16)

        def step(i, _):
            j, c = i // 2, i % 2
            source = act[c, :, j].reshape(288, 512)
            put = dot_n(matrix, source).astype(BF16)
            for k in range(5):
                h = HALF[k]
                at = pl.multiple_of(BASE[k] + j * (2 * h), 2 * h)
                acts[c, pl.ds(at, 2 * h), :] = put[2 * OFF[k] : 2 * OFF[k] + 2 * h]
            return 0

        lax.fori_loop(0, 16, step, 0)

    def score(m):
        at = pl.multiple_of(m * 256, 256)
        lhs = rows[pl.ds(at, 256), :]

        def step(i, total):
            c, n = i // 2, pl.multiple_of((i % 2) * 256, 256)
            got = dot_t(lhs, wd[c, pl.ds(n, 256), :])
            prod = got * acts[c, pl.ds(at, 256), pl.ds(n, 256)].astype(F32)
            return total + prod[:, :128] + prod[:, 128:]

        total = lax.fori_loop(0, 4, step, jnp.zeros((256, 128), F32))
        scores[pl.ds(m, 1), :] = jnp.sum(total.T, axis=0, keepdims=True)

    def score_chunk(k):
        relayed(k)
        if k == 0:
            score(0)
        else:
            lax.fori_loop(2 * k - 1, 2 * k + 1, lambda m, _: (score(m), 0)[1], 0)
        for j in range(8):
            n = 2 * HALF[k]
            m, at = (0, 32 * j) if k == 0 else (2 * k - 1 + j // 4, 64 * (j % 4))
            sent[j, k : k + 1, 0:n] = scores[m : m + 1, at : at + n]

    others = [(dy, dx) for dy in (0, 1) for dx in range(4) if dy or dx]
    toward = lambda dy, dx: ((yh + dy) % 2, (x + dx) % 4)

    def to_chips(tag, src_of, dst):
        for dy, dx in others:
            y_, x_ = toward(dy, dx)
            start(f"{tag}{dy}{dx}", src_of(y_ * 4 + x_), dst.at[mine], (plane(y_, x_), e))

    def from_chips(tag, dst):
        for dy, dx in others:
            y_, x_ = toward(dy, 4 - dx)
            arrived(f"{tag}{dy}{dx}", dst.at[y_ * 4 + x_])

    def summarize():
        total = shard_summary(inner, c_in, cum)
        pair[core] = total
        start("pair", pair.at[core], pair.at[core], sib)

    def combine_pair():
        arrived("pair", pair.at[1 - core])
        grown = jnp.exp(pair[0, 16:17])
        chips[mine, 0:16] = pair[0, 0:16] + grown * pair[1, 0:16]
        chips[mine, 16:24] = pair[0, 16:24] + pair[1, 16:24]
        to_chips("st", lambda j: chips.at[mine], chips)

    def entering():
        from_chips("st", chips)

        def enter(n, state):
            k = 7 - n
            got = chips[k]
            return jnp.where(k > mine, got[0:16] + jnp.exp(got[16:17]) * state, state)

        state = lax.fori_loop(0, 8, enter, jnp.zeros((16, 256), F32))
        later = pair[1]
        return jnp.where(core == 0, later[0:16] + jnp.exp(later[16:17]) * state, state)

    def finish():
        to_chips("sc", lambda j: sent.at[j], parts)
        named = ids[:, pl.ds(pl.multiple_of(e * 128, 128), 128)]
        expert = lax.broadcasted_iota(jnp.int32, (16, 128), 0)
        hit = (named[0:1] == expert) | (named[1:2] == expert)
        lower = lax.broadcasted_iota(jnp.int32, (128, 128), 0)
        along = lax.broadcasted_iota(jnp.int32, (128, 128), 1)
        upto = jnp.where(lower <= along, 1.0, 0.0).astype(BF16)
        slot = dot_n(jnp.where(hit, 1.0, 0.0).astype(BF16), upto).astype(jnp.int32) - 1
        off = (z - (expert & 7) + 8) & 7
        place = 18 * jnp.where(off < 4, 2 * off, 15 - 2 * off) + slot
        first = place < 16
        chunk = jnp.where(first, 0, 1 + ((place - 16) >> 5))
        spot_ = jnp.where(first, place, (place - 16) & 31)
        lane = spot_ + jnp.where((expert >> 3) == yl, 0, jnp.where(first, 16, 32))
        from_chips("sc", parts)
        total = sent[mine]
        for dy, dx in others:
            y_, x_ = toward(dy, dx)
            total = total + parts[y_ * 4 + x_]
        tables[e] = total
        for d in range(1, 16):
            start(f"ex{d}", tables.at[e], tables.at[e], (s, (e + d) % 16))
        for d in range(1, 16):
            arrived(f"ex{d}", tables.at[(e + 16 - d) % 16])
        row8 = lax.broadcasted_iota(jnp.int32, (8, 128), 0)
        lines = [jnp.zeros((1, 128), F32), jnp.zeros((1, 128), F32)]
        for i in range(16):
            table = tables[i]
            hi = table.astype(BF16)
            mid, low = halves(table - hi.astype(F32))
            chosen = jnp.where(lower == lane[i : i + 1], 1.0, 0.0).astype(BF16)
            got = dot_n(jnp.concatenate([hi.astype(F32), mid.astype(F32), low.astype(F32)], axis=0).astype(BF16), chosen)
            got = (got[16:24] + got[8:16]) + got[0:8]
            got = jnp.sum(jnp.where(row8 == chunk[i : i + 1], got, 0.0), axis=0, keepdims=True)
            for k in (0, 1):
                lines[k] = jnp.where(named[k : k + 1] == i, got, lines[k])
        gate[...] = jnp.concatenate(lines, axis=0)

    sent[...] = jnp.zeros_like(sent)
    pick_and_send(0)
    chunk_decays(ld, cum, cum_t)
    turn_steps(st, step_t)
    spread(0)
    ring(1)
    pick_and_send(1)
    arrived("w", proj.at[1 - yl, part_of_w])
    start("wf", proj.at[1 - yl, part_of_w], proj.at[1 - yl, part_of_w], sib)
    ordered()
    spread(1)
    ring(2)
    pick_and_send(2)
    arrived("wf", proj.at[1 - yl, rest_of_w])
    for a in range(3):
        product(a)
    spread(2)
    relay(0)
    ring(3)
    pick_and_send(3)
    for a in range(3, 5):
        product(a)
    spread(3)
    relay(1)
    ring(4)
    pick_and_send(4)
    for a in range(5, 8):
        product(a)
    spread(4)
    relay(2)
    for a in range(8):
        to = pl.ds(pl.multiple_of(((1 - yl) * 8 + spot(a)) * 128, 128), 128)
        arrived(f"c{a}", inner.at[to])
    summarize()
    loads[2].wait()
    arrived("wd", wd.at[1 - core])
    score_chunk(0)
    combine_pair()
    score_chunk(1)
    relay(3)
    sweep(inner, b_in, c_in, gain, out, cum, cum_t, step_t, entering())
    relay(4)
    score_chunk(2)
    score_chunk(3)
    score_chunk(4)
    finish()
    for copy in pending:
        copy.wait_send()


def chunk_decays(ld, cum, cum_t):
    lines = [
        jnp.concatenate([ld[:, 128 * i : 128 * (i + 1)], jnp.zeros((4, 128), F32)], axis=0)
        for i in range(16)
    ]
    x = jnp.concatenate(lines, axis=0)
    hi, rest = x.astype(BF16), None
    rest = x - hi.astype(F32)
    mid, low = halves(rest)
    tri = lax.broadcasted_iota(jnp.int32, (128, 128), 0) <= lax.broadcasted_iota(
        jnp.int32, (128, 128), 1
    )
    tri = jnp.where(tri, 1.0, 0.0).astype(BF16)
    total = (dot_n(low, tri) + dot_n(mid, tri)) + dot_n(hi, tri)
    for i in range(16):
        cum[i] = total[8 * i : 8 * i + 8]
    if cum_t is not None:
        turned = total.T
        for i in range(16):
            cum_t[i] = turned[:, 8 * i : 8 * i + 8]


def by_head(values):
    lane = lax.broadcasted_iota(jnp.int32, (1, 256), 1) // HEAD
    out = jnp.broadcast_to(values[3], (1, 256))
    for i in (2, 1, 0):
        out = jnp.where(lane == i, jnp.broadcast_to(values[i], (1, 256)), out)
    return out


def chunk_state(inner, c_in, cum, i):
    at = pl.ds(pl.multiple_of(i * 128, 128), 128)
    grown = jnp.exp(cum[i])
    c = c_in[:, at]
    hi, low = halves(jnp.concatenate([c * grown[h : h + 1] for h in range(4)], axis=0))
    g_hi, g_low = halves(inner[at, :])
    left = jnp.concatenate([hi, low, hi], axis=1)
    right = jnp.concatenate([g_hi, g_hi, g_low], axis=0)
    full = dot_n(left, right)
    lane = lax.broadcasted_iota(jnp.int32, (16, 256), 1) // HEAD
    out = full[48:64]
    for h in (2, 1, 0):
        out = jnp.where(lane == h, full[16 * h : 16 * h + 16], out)
    return out


def chunk_total(cum, i):
    ends = cum[i]
    return by_head([ends[h : h + 1, 127:128] for h in range(4)])


def shard_summary(inner, c_in, cum):
    def step(n, carry):
        state, total = carry
        i = 15 - n
        ends = chunk_total(cum, i)
        return chunk_state(inner, c_in, cum, i) + jnp.exp(ends) * state, total + ends

    state, total = lax.fori_loop(
        0, 16, step, (jnp.zeros((16, 256), F32), jnp.zeros((1, 256), F32)), unroll=2
    )
    return jnp.concatenate([state, jnp.broadcast_to(total, (8, 256))], axis=0)


def turn_steps(st, step_t):
    lines = [
        jnp.concatenate([st[:, 128 * i : 128 * (i + 1)], jnp.zeros((4, 128), F32)], axis=0)
        for i in range(16)
    ]
    turned = jnp.concatenate(lines, axis=0).T
    for i in range(16):
        step_t[i] = turned[:, 8 * i : 8 * i + 8]


def sweep(inner, b_in, c_in, gain, out, cum, cum_t, step_t, state):
    upper = lax.broadcasted_iota(jnp.int32, (128, 128), 1) >= lax.broadcasted_iota(
        jnp.int32, (128, 128), 0
    )
    left_lanes = lax.broadcasted_iota(jnp.int32, (128, 128), 1) < HEAD
    gains = gain[...]

    def step(n, state):
        i = 15 - n
        at = pl.ds(pl.multiple_of(i * 128, 128), 128)
        b_hi, b_low = halves(b_in[:, at])
        c_hi, c_low = halves(c_in[:, at])
        b_all = jnp.concatenate([b_hi, b_low, b_hi], axis=0)
        table = dot_tn(b_all, jnp.concatenate([c_hi, c_hi, c_low], axis=0))
        s_hi, s_low = halves(state)
        carried = dot_tn(b_all, jnp.concatenate([s_hi, s_hi, s_low], axis=0))
        rows_, cols, steps = cum[i], cum_t[i], step_t[i]
        for p in (0, 1):
            lanes = slice(128 * p, 128 * p + 128)
            g = inner[at, lanes]
            tail, size = [], []
            m_hi, m_low = [], []
            for h in (2 * p, 2 * p + 1):
                col = jnp.broadcast_to(cols[:, h : h + 1], (128, 128))
                row = rows_[h : h + 1]
                gap = jnp.where(upper, row - col, 0.0)
                weight = jnp.where(upper, jnp.exp(gap), 0.0) * table
                hi, low = halves(weight)
                m_hi.append(hi)
                m_low.append(low)
                tail.append(jnp.exp(row[:, 127:128] - col))
                size.append(jnp.broadcast_to(steps[:, h : h + 1], (128, 128)))
            g_a, g_b = halves(jnp.where(left_lanes, g, 0.0)), halves(jnp.where(left_lanes, 0.0, g))
            left = jnp.concatenate(m_hi + m_low + m_hi, axis=1)
            right = jnp.concatenate([g_a[0], g_b[0], g_a[0], g_b[0], g_a[1], g_b[1]], axis=0)
            within = dot_n(left, right)
            tails = jnp.where(left_lanes, tail[0], tail[1])
            sizes = jnp.where(left_lanes, size[0], size[1])
            value = sizes * (within + carried[:, lanes] * tails) + gains[:, lanes] * g
            out[at, lanes] = value.astype(BF16)
        return chunk_state(inner, c_in, cum, i) + jnp.exp(chunk_total(cum, i)) * state

    lax.fori_loop(0, 16, step, state)


def shards(
    grad_out, out_proj, step_size, log_decay, b_input, c_output,
    skip_gain, expert_ids, hidden_act, w_down,
):
    hidden = hidden_act[0].transpose(1, 0, 2).reshape(18, 8, 2, 16, 512)
    return pl.pallas_call(
        comm_kernel,
        name="mixer_and_router",
        out_shape=(
            jax.ShapeDtypeStruct((2048, 256), BF16),
            jax.ShapeDtypeStruct((2, 128), F32),
        ),
        in_specs=[HBM_ANY, HBM_ANY, VMEM_ANY, HBM_ANY, HBM_ANY] + [VMEM_ANY] * 5,
        out_specs=(VMEM_ANY, VMEM_ANY),
        scratch_shapes=[
            pltpu.VMEM((2048, 256), F32),
            pltpu.VMEM((8, 128, 2048), BF16),
            pltpu.VMEM((2, 256, 2048), BF16),
            pltpu.VMEM((8, 128, 256), F32),
            pltpu.VMEM((2304, 2048), BF16),
            pltpu.VMEM((144, 2048), BF16),
            pltpu.VMEM((2, 512, 2048), BF16),
            pltpu.VMEM((2, 18, 8, 16, 512), BF16),
            pltpu.VMEM((2, 2304, 512), BF16),
            pltpu.VMEM((16, 128), F32),
            pltpu.VMEM((9, 256), F32),
            pltpu.VMEM((8, 8, 128), F32),
            pltpu.VMEM((8, 8, 128), F32),
            pltpu.VMEM((16, 8, 128), F32),
            pltpu.VMEM((16, 8, 128), F32),
            pltpu.VMEM((16, 128, 8), F32),
            pltpu.VMEM((16, 128, 8), F32),
            pltpu.VMEM((2, 24, 256), F32),
            pltpu.VMEM((8, 24, 256), F32),
            pltpu.SemaphoreType.DMA((112,)),
            pltpu.SemaphoreType.DMA((112,)),
            pltpu.SemaphoreType.DMA((4,)),
        ],
        compiler_params=pltpu.CompilerParams(
            collective_id=0, has_side_effects=True, vmem_limit_bytes=60 * 1024 * 1024
        ),
    )(
        grad_out, out_proj, expert_ids.T, hidden, w_down[0],
        log_decay, step_size, b_input, c_output, skip_gain.reshape(1, 256),
    )


def solution(mesh):
    in_specs = (
        P(("seq", "exp"), None),
        P("exp", None),
        P("exp", "seq"),
        P("exp", "seq"),
        P(None, "seq"),
        P(None, "seq"),
        P("exp"),
        P("seq", None),
        P("exp", None, None, "seq"),
        P("exp", "seq", None),
    )
    out_specs = (P("seq", "exp"), P(None, ("seq", "exp")))
    return jax.shard_map(shards, mesh=mesh, in_specs=in_specs, out_specs=out_specs, check_vma=False)
```

```python
import jax
import jax.numpy as jnp
from jax import lax
from jax.experimental import pallas as pl
from jax.experimental.pallas import tpu as pltpu
from jax.sharding import PartitionSpec as P

HEAD = 64
MESH = pl.DeviceIdType.MESH
F32, BF16 = jnp.float32, jnp.bfloat16

CAP = 18
HALF = (16, 32, 32, 32, 16, 16)
OFF = (0, 16, 48, 80, 112, 128)
BASE = (0, 256, 768, 1280, 1792, 2048)
CHUNKS = len(HALF)
RANK = (0, -1, 1, -2, 2, -3, 3, 4)
VMEM_ANY = pl.BlockSpec(memory_space=pltpu.VMEM)
HBM_ANY = pl.BlockSpec(memory_space=pl.ANY)


def dot_t(a, b):
    return lax.dot_general(a, b, (((1,), (1,)), ((), ())), preferred_element_type=F32)


def dot_n(a, b):
    return lax.dot_general(a, b, (((1,), (0,)), ((), ())), preferred_element_type=F32)


def dot_tn(a, b):
    return lax.dot_general(a, b, (((0,), (0,)), ((), ())), preferred_element_type=F32)


def halves(x):
    hi = x.astype(BF16)
    return hi, (x - hi.astype(F32)).astype(BF16)


def order_matrix(z, yl):
    row = lax.broadcasted_iota(jnp.int32, (288, 288), 0)
    col = lax.broadcasted_iota(jnp.int32, (288, 288), 1)
    late, last = row - 32, row - 224
    side = jnp.where(row < 32, row >> 4, jnp.where(row < 224, (late >> 5) & 1, (last >> 4) & 1))
    middle = jnp.where(
        row < 224, 16 + ((late >> 6) << 5) + (late & 31), 112 + ((last >> 5) << 4) + (last & 15)
    )
    place = jnp.where(row < 32, row & 15, middle)
    arrival = (place * 3641) >> 16
    slot = place - 18 * arrival
    shift = jnp.where((arrival & 1) == 1, -((arrival + 1) >> 1), arrival >> 1)
    source = (z + shift) & 7
    lane = jnp.where(side == 0, yl, 1 - yl)
    return col == slot * 16 + lane * 8 + source


def comm_kernel(
    g_hbm, w_hbm, ids, hid, wd_hbm, ld, st, b_in, c_in, gain, out, gate,
    inner, blocks, proj, outbox, rows, picks, wd, act, acts, keys, scores, sent, parts, tables,
    cum, cum_t, step_t, states, pair, chips, send, recv, local,
):
    s, e = lax.axis_index("seq"), lax.axis_index("exp")
    core, x, yh = s % 2, (s // 2) % 4, s // 8
    z, yl = e % 8, e // 8
    mine, other = yh * 4 + x, (1 - yh) * 4 + x
    plane = lambda yh_, x_: (yh_ * 4 + x_) * 2 + core
    zp, zm = (s, yl * 8 + (z + 1) % 8), (s, yl * 8 + (z + 7) % 8)
    xp, xm = (plane(yh, (x + 1) % 4), e), (plane(yh, (x + 3) % 4), e)
    yp, yq = (s, (1 - yl) * 8 + z), (plane(1 - yh, x), e)
    yd = (plane(1 - yh, x), (1 - yl) * 8 + z)
    sib = ((yh * 4 + x) * 2 + 1 - core, e)
    peers = (zp, zm, xp, xm, yp, yq, yd, sib)
    names, pending = {}, []

    def start(name, src, dst, to):
        i = names.setdefault(name, len(names))
        copy = pltpu.make_async_remote_copy(
            src_ref=src, dst_ref=dst, send_sem=send.at[i], recv_sem=recv.at[i],
            device_id=to, device_id_type=MESH,
        )
        copy.start()
        pending.append(copy)

    def arrived(name, dst):
        i = names[name]
        pltpu.make_async_remote_copy(
            src_ref=dst, dst_ref=dst, send_sem=send.at[i], recv_sem=recv.at[i],
            device_id=sib, device_id_type=MESH,
        ).wait_recv()

    def part(k, j, side=None):
        h = HALF[k]
        at = pl.multiple_of(BASE[k] + j * (2 * h), 2 * h)
        if side is None:
            return rows.at[pl.ds(at, 2 * h)]
        return rows.at[pl.ds(pl.multiple_of(at + side * h, 16), h)]

    spot = lambda a: (z + RANK[a] + 8) % 8
    loads = [
        pltpu.make_async_copy(g_hbm, blocks.at[z], local.at[0]),
        pltpu.make_async_copy(w_hbm, proj.at[yl], local.at[1]),
        pltpu.make_async_copy(wd_hbm, wd.at[core], local.at[2]),
        pltpu.make_async_copy(hid.at[:, :, core], act.at[core], local.at[3]),
    ]
    for load in loads:
        load.start()
    barrier = pltpu.get_barrier_semaphore()
    for peer in peers:
        pl.semaphore_signal(barrier, inc=1, device_id=peer, device_id_type=MESH)
    pl.semaphore_wait(barrier, len(peers))

    loads[0].wait()
    start("zp0", blocks.at[z], blocks.at[z], zp)
    start("zm0", blocks.at[z], blocks.at[z], zm)
    part_of_w = pl.ds(pl.multiple_of(core * 128, 128), 128)
    rest_of_w = pl.ds(pl.multiple_of((1 - core) * 128, 128), 128)
    loads[1].wait()
    start("wd", wd_hbm, wd.at[core], sib)
    start("hid", hid.at[:, :, 1 - core], act.at[core], sib)

    for a in range(8):
        lanes = pl.ds(pl.multiple_of((yl * 8 + spot(a)) * 128, 128), 128)
        named = ids[:, lanes]
        for side, expert in ((0, e), (1, (1 - yl) * 8 + z)):
            hit = (named[0:1] == expert) | (named[1:2] == expert)
            keys[2 * a + side : 2 * a + side + 1, :] = jnp.where(hit, 1.0, 0.0)
    hits = keys[...]
    tri = lax.broadcasted_iota(jnp.int32, (128, 128), 0) <= lax.broadcasted_iota(
        jnp.int32, (128, 128), 1
    )
    rank = dot_n(hits.astype(BF16), jnp.where(tri, 1.0, 0.0).astype(BF16))
    keys[...] = jnp.where(hits > 0.5, rank - 1.0, -1000.0)

    def pick(k):
        h = HALF[k]
        place = lax.broadcasted_iota(jnp.int32, (h, 128), 0) + OFF[k]
        first, last = OFF[k] // CAP, (OFF[k] + h - 1) // CAP
        wanted = []
        for a in range(first, last + 1):
            at = (place - CAP * a).astype(F32)
            sides = [keys[2 * a + side : 2 * a + side + 1, :] == at for side in (0, 1)]
            wanted.append(
                jnp.concatenate([jnp.where(m, 1.0, 0.0) for m in sides], axis=0).astype(BF16)
            )
        for n in range(0, 2048, 512):
            found = None
            for a, chosen in zip(range(first, last + 1), wanted):
                more = dot_n(chosen, blocks[spot(a), :, n : n + 512])
                found = more if found is None else found + more
            found = found.astype(BF16)
            at = pl.multiple_of(BASE[k] + mine * (2 * h), 2 * h)
            rows[pl.ds(at, h), n : n + 512] = found[:h]
            picks[OFF[k] : OFF[k] + h, n : n + 512] = found[h:]

    def pick_and_send(k):
        pick(k)
        cut = picks.at[OFF[k] : OFF[k] + HALF[k]]
        start(f"pl{k}", cut, part(k, mine, 1), yp)
        start(f"pd{k}", cut, part(k, mine, 1), yd)
        start(f"ow{k}", part(k, mine, 0), part(k, mine, 0), yq)
        to_both("a", k, mine, 0)

    def to_both(tag, k, j, side):
        start(f"xp{tag}{side}{k}", part(k, j, side), part(k, j, side), xp)
        start(f"xm{tag}{side}{k}", part(k, j, side), part(k, j, side), xm)

    def spread(k):
        arrived(f"pl{k}", part(k, mine, 1))
        to_both("a", k, mine, 1)
        arrived(f"pd{k}", part(k, other, 1))
        to_both("b", k, other, 1)
        arrived(f"ow{k}", part(k, other, 0))
        to_both("b", k, other, 0)

    def relay(k):
        for tag, side in (("a", yh), ("b", 1 - yh)):
            before, after = side * 4 + (x + 3) % 4, side * 4 + (x + 1) % 4
            arrived(f"xp{tag}0{k}", part(k, before, 0))
            start(f"fp{tag}{k}", part(k, before, 0), part(k, before, 0), xp)
            arrived(f"xm{tag}1{k}", part(k, after, 1))
            start(f"fm{tag}{k}", part(k, after, 1), part(k, after, 1), xm)

    def relayed(k):
        for tag, side in (("a", yh), ("b", 1 - yh)):
            before, after = side * 4 + (x + 3) % 4, side * 4 + (x + 1) % 4
            far = side * 4 + (x + 2) % 4
            arrived(f"xp{tag}1{k}", part(k, before, 1))
            arrived(f"xm{tag}0{k}", part(k, after, 0))
            arrived(f"fp{tag}{k}", part(k, far, 0))
            arrived(f"fm{tag}{k}", part(k, far, 1))

    def ring(k):
        back, ahead = (z - k + 8) % 8, (z + k) % 8
        if k < 4:
            arrived(f"zp{k - 1}", blocks.at[back])
            arrived(f"zm{k - 1}", blocks.at[ahead])
        else:
            arrived("zp3", blocks.at[back, 0:64])
            arrived("zm3", blocks.at[ahead, 64:128])
        if k < 3:
            start(f"zp{k}", blocks.at[back], blocks.at[back], zp)
            start(f"zm{k}", blocks.at[ahead], blocks.at[ahead], zm)
        elif k == 3:
            start("zp3", blocks.at[back, 0:64], blocks.at[back, 0:64], zp)
            start("zm3", blocks.at[ahead, 64:128], blocks.at[ahead, 64:128], zm)

    def product(a):
        block = blocks[spot(a)]
        outbox[a] = dot_t(block, proj[1 - yl])
        to = pl.ds(pl.multiple_of((yl * 8 + spot(a)) * 128, 128), 128)
        start(f"c{a}", outbox.at[a], inner.at[to], yp)
        inner[to, :] = dot_t(block, proj[yl])

    def ordered():
        loads[3].wait()
        arrived("hid", act.at[1 - core])
        matrix = jnp.where(order_matrix(z, yl), 1.0, 0.0).astype(BF16)

        def step(i, _):
            j, c = i // 2, i % 2
            source = act[c, :, j].reshape(288, 512)
            put = dot_n(matrix, source).astype(BF16)
            for k in range(CHUNKS):
                h = HALF[k]
                at = pl.multiple_of(BASE[k] + j * (2 * h), 2 * h)
                acts[c, pl.ds(at, 2 * h), :] = put[2 * OFF[k] : 2 * OFF[k] + 2 * h]
            return 0

        lax.fori_loop(0, 16, step, 0)

    def score(m):
        at = pl.multiple_of(m * 256, 256)
        lhs = rows[pl.ds(at, 256), :]

        def step(i, total):
            c, n = i // 2, pl.multiple_of((i % 2) * 256, 256)
            got = dot_t(lhs, wd[c, pl.ds(n, 256), :])
            prod = got * acts[c, pl.ds(at, 256), pl.ds(n, 256)].astype(F32)
            return total + prod[:, :128] + prod[:, 128:]

        total = lax.fori_loop(0, 4, step, jnp.zeros((256, 128), F32))
        scores[pl.ds(m, 1), :] = jnp.sum(total.T, axis=0, keepdims=True)

    def score_chunk(k):
        relayed(k)
        n, m = 2 * HALF[k], BASE[k] // 256
        if n == 32:
            score(m)
        else:
            lax.fori_loop(m, m + 2, lambda i, _: (score(i), 0)[1], 0)
        for j in range(8):
            at = n * j
            sent[j, k : k + 1, 0:n] = scores[m + at // 256 : m + at // 256 + 1, at % 256 : at % 256 + n]

    others = [(dy, dx) for dy in (0, 1) for dx in range(4) if dy or dx]
    toward = lambda dy, dx: ((yh + dy) % 2, (x + dx) % 4)

    def to_chips(tag, src_of, dst):
        for dy, dx in others:
            y_, x_ = toward(dy, dx)
            start(f"{tag}{dy}{dx}", src_of(y_ * 4 + x_), dst.at[mine], (plane(y_, x_), e))

    def from_chips(tag, dst):
        for dy, dx in others:
            y_, x_ = toward(dy, 4 - dx)
            arrived(f"{tag}{dy}{dx}", dst.at[y_ * 4 + x_])

    def chunk_of(a, side):
        shift = (a // 2) * (1 - 2 * (a % 2)) - a % 2
        return side * 8 + (z + shift + 8) % 8

    def own_part(first, last):
        for a in range(first, last):
            product(a)
        lax.fori_loop(first, last, lambda a, _: local_chunk(chunk_of(a, yl)), 0)

    def other_part(first, last):
        for a in range(first, last):
            to = pl.ds(pl.multiple_of(((1 - yl) * 8 + spot(a)) * 128, 128), 128)
            arrived(f"c{a}", inner.at[to])
        lax.fori_loop(first, last, lambda a, _: local_chunk(chunk_of(a, 1 - yl)), 0)

    def local_chunk(i):
        states[i] = chunk_state(inner, c_in, cum, i)
        within_chunk(inner, b_in, c_in, gain, cum, cum_t, step_t, i)
        return 0

    def summarize():
        total = shard_summary(states, cum)
        pair[core] = total
        start("pair", pair.at[core], pair.at[core], sib)

    def combine_pair():
        arrived("pair", pair.at[1 - core])
        grown = jnp.exp(pair[0, 16:17])
        chips[mine, 0:16] = pair[0, 0:16] + grown * pair[1, 0:16]
        chips[mine, 16:24] = pair[0, 16:24] + pair[1, 16:24]
        to_chips("st", lambda j: chips.at[mine], chips)

    def entering():
        from_chips("st", chips)

        def enter(n, state):
            k = 7 - n
            got = chips[k]
            return jnp.where(k > mine, got[0:16] + jnp.exp(got[16:17]) * state, state)

        state = lax.fori_loop(0, 8, enter, jnp.zeros((16, 256), F32))
        later = pair[1]
        return jnp.where(core == 0, later[0:16] + jnp.exp(later[16:17]) * state, state)

    def finish():
        to_chips("sc", lambda j: sent.at[j], parts)
        sweep(inner, b_in, out, cum, cum_t, step_t, states, entering())
        named = ids[:, pl.ds(pl.multiple_of(e * 128, 128), 128)]
        expert = lax.broadcasted_iota(jnp.int32, (16, 128), 0)
        hit = (named[0:1] == expert) | (named[1:2] == expert)
        lower = lax.broadcasted_iota(jnp.int32, (128, 128), 0)
        along = lax.broadcasted_iota(jnp.int32, (128, 128), 1)
        upto = jnp.where(lower <= along, 1.0, 0.0).astype(BF16)
        slot = dot_n(jnp.where(hit, 1.0, 0.0).astype(BF16), upto).astype(jnp.int32) - 1
        off = (z - (expert & 7) + 8) & 7
        place = 18 * jnp.where(off < 4, 2 * off, 15 - 2 * off) + slot
        wide = (place >= 16) & (place < 112)
        chunk = jnp.where(wide, 1 + ((place - 16) >> 5), jnp.where(place < 16, 0, 4 + ((place - 112) >> 4)))
        spot_ = jnp.where(wide, (place - 16) & 31, place & 15)
        lane = spot_ + jnp.where((expert >> 3) == yl, 0, jnp.where(wide, 32, 16))
        from_chips("sc", parts)
        total = sent[mine]
        for dy, dx in others:
            y_, x_ = toward(dy, dx)
            total = total + parts[y_ * 4 + x_]
        tables[e] = total
        for d in range(1, 16):
            start(f"ex{d}", tables.at[e], tables.at[e], (s, (e + d) % 16))
        for d in range(1, 16):
            arrived(f"ex{d}", tables.at[(e + 16 - d) % 16])
        row8 = lax.broadcasted_iota(jnp.int32, (8, 128), 0)
        lines = [jnp.zeros((1, 128), F32), jnp.zeros((1, 128), F32)]
        for i in range(16):
            table = tables[i]
            hi = table.astype(BF16)
            mid, low = halves(table - hi.astype(F32))
            chosen = jnp.where(lower == lane[i : i + 1], 1.0, 0.0).astype(BF16)
            got = dot_n(jnp.concatenate([hi.astype(F32), mid.astype(F32), low.astype(F32)], axis=0).astype(BF16), chosen)
            got = (got[16:24] + got[8:16]) + got[0:8]
            got = jnp.sum(jnp.where(row8 == chunk[i : i + 1], got, 0.0), axis=0, keepdims=True)
            for k in (0, 1):
                lines[k] = jnp.where(named[k : k + 1] == i, got, lines[k])
        gate[...] = jnp.concatenate(lines, axis=0)

    def send_w(n):
        at = pl.ds(pl.multiple_of(core * 128 + 64 * n, 64), 64)
        start(f"w{n}", proj.at[yl, at], proj.at[yl, at], yd)

    pick_and_send(0)
    send_w(0)
    sent[...] = jnp.zeros_like(sent)
    spread(0)
    chunk_decays(ld, cum, cum_t)
    turn_steps(st, step_t)
    ring(1)
    pick_and_send(1)
    send_w(1)
    ordered()
    spread(1)
    ring(2)
    pick_and_send(2)
    for n in (0, 1):
        arrived(f"w{n}", proj.at[1 - yl, pl.ds(pl.multiple_of(core * 128 + 64 * n, 64), 64)])
    start("wf", proj.at[1 - yl, part_of_w], proj.at[1 - yl, part_of_w], sib)
    relay(0)
    spread(2)
    arrived("wf", proj.at[1 - yl, rest_of_w])
    own_part(0, 3)
    ring(3)
    pick_and_send(3)
    relay(1)
    spread(3)
    own_part(3, 5)
    ring(4)
    pick_and_send(4)
    pick_and_send(5)
    spread(4)
    spread(5)
    own_part(5, 8)
    other_part(0, 3)
    relay(2)
    other_part(3, 5)
    loads[2].wait()
    arrived("wd", wd.at[1 - core])
    score_chunk(0)
    score_chunk(1)
    relay(3)
    other_part(5, 8)
    summarize()
    score_chunk(2)
    combine_pair()
    relay(4)
    relay(5)
    score_chunk(3)
    score_chunk(4)
    score_chunk(5)
    finish()
    for copy in pending:
        copy.wait_send()


def chunk_decays(ld, cum, cum_t):
    lines = [
        jnp.concatenate([ld[:, 128 * i : 128 * (i + 1)], jnp.zeros((4, 128), F32)], axis=0)
        for i in range(16)
    ]
    x = jnp.concatenate(lines, axis=0)
    hi, rest = x.astype(BF16), None
    rest = x - hi.astype(F32)
    mid, low = halves(rest)
    tri = lax.broadcasted_iota(jnp.int32, (128, 128), 0) <= lax.broadcasted_iota(
        jnp.int32, (128, 128), 1
    )
    tri = jnp.where(tri, 1.0, 0.0).astype(BF16)
    total = (dot_n(low, tri) + dot_n(mid, tri)) + dot_n(hi, tri)
    for i in range(16):
        cum[i] = total[8 * i : 8 * i + 8]
    if cum_t is not None:
        turned = total.T
        for i in range(16):
            cum_t[i] = turned[:, 8 * i : 8 * i + 8]


def by_head(values):
    lane = lax.broadcasted_iota(jnp.int32, (1, 256), 1) // HEAD
    out = jnp.broadcast_to(values[3], (1, 256))
    for i in (2, 1, 0):
        out = jnp.where(lane == i, jnp.broadcast_to(values[i], (1, 256)), out)
    return out


def chunk_state(inner, c_in, cum, i):
    at = pl.ds(pl.multiple_of(i * 128, 128), 128)
    grown = jnp.exp(cum[i])
    c = c_in[:, at]
    hi, low = halves(jnp.concatenate([c * grown[h : h + 1] for h in range(4)], axis=0))
    g_hi, g_low = halves(inner[at, :])
    left = jnp.concatenate([hi, low, hi], axis=1)
    right = jnp.concatenate([g_hi, g_hi, g_low], axis=0)
    full = dot_n(left, right)
    lane = lax.broadcasted_iota(jnp.int32, (16, 256), 1) // HEAD
    out = full[48:64]
    for h in (2, 1, 0):
        out = jnp.where(lane == h, full[16 * h : 16 * h + 16], out)
    return out


def chunk_total(cum, i):
    ends = cum[i]
    return by_head([ends[h : h + 1, 127:128] for h in range(4)])


def shard_summary(states, cum):
    def step(n, carry):
        state, total = carry
        ends = chunk_total(cum, 15 - n)
        return states[15 - n] + jnp.exp(ends) * state, total + ends

    state, total = lax.fori_loop(
        0, 16, step, (jnp.zeros((16, 256), F32), jnp.zeros((1, 256), F32)), unroll=4
    )
    return jnp.concatenate([state, jnp.broadcast_to(total, (8, 256))], axis=0)


def turn_steps(st, step_t):
    lines = [
        jnp.concatenate([st[:, 128 * i : 128 * (i + 1)], jnp.zeros((4, 128), F32)], axis=0)
        for i in range(16)
    ]
    turned = jnp.concatenate(lines, axis=0).T
    for i in range(16):
        step_t[i] = turned[:, 8 * i : 8 * i + 8]


def within_chunk(inner, b_in, c_in, gain, cum, cum_t, step_t, i):
    upper = lax.broadcasted_iota(jnp.int32, (128, 128), 1) >= lax.broadcasted_iota(
        jnp.int32, (128, 128), 0
    )
    left_lanes = lax.broadcasted_iota(jnp.int32, (128, 128), 1) < HEAD
    gains = gain[...]
    at = pl.ds(pl.multiple_of(i * 128, 128), 128)
    b_hi, b_low = halves(b_in[:, at])
    c_hi, c_low = halves(c_in[:, at])
    b_all = jnp.concatenate([b_hi, b_low, b_hi], axis=0)
    table = dot_tn(b_all, jnp.concatenate([c_hi, c_hi, c_low], axis=0))
    rows_, cols, steps = cum[i], cum_t[i], step_t[i]
    for p in (0, 1):
        lanes = slice(128 * p, 128 * p + 128)
        g = inner[at, lanes]
        size, m_hi, m_low = [], [], []
        for h in (2 * p, 2 * p + 1):
            col = jnp.broadcast_to(cols[:, h : h + 1], (128, 128))
            gap = jnp.where(upper, rows_[h : h + 1] - col, 0.0)
            weight = jnp.where(upper, jnp.exp(gap), 0.0) * table
            hi, low = halves(weight)
            m_hi.append(hi)
            m_low.append(low)
            size.append(jnp.broadcast_to(steps[:, h : h + 1], (128, 128)))
        g_a, g_b = halves(jnp.where(left_lanes, g, 0.0)), halves(jnp.where(left_lanes, 0.0, g))
        left = jnp.concatenate(m_hi + m_low + m_hi, axis=1)
        right = jnp.concatenate([g_a[0], g_b[0], g_a[0], g_b[0], g_a[1], g_b[1]], axis=0)
        sizes = jnp.where(left_lanes, size[0], size[1])
        inner[at, lanes] = sizes * dot_n(left, right) + gains[:, lanes] * g


def sweep(local, b_in, out, cum, cum_t, step_t, states, state):
    left_lanes = lax.broadcasted_iota(jnp.int32, (128, 128), 1) < HEAD

    def step(n, state):
        i = 15 - n
        at = pl.ds(pl.multiple_of(i * 128, 128), 128)
        b_hi, b_low = halves(b_in[:, at])
        s_hi, s_low = halves(state)
        carried = dot_tn(
            jnp.concatenate([b_hi, b_low, b_hi], axis=0),
            jnp.concatenate([s_hi, s_hi, s_low], axis=0),
        )
        ends, cols, steps = cum[i][:, 127:128], cum_t[i], step_t[i]
        for p in (0, 1):
            lanes = slice(128 * p, 128 * p + 128)
            scale = [
                jnp.broadcast_to(
                    steps[:, h : h + 1] * jnp.exp(ends[h : h + 1] - cols[:, h : h + 1]), (128, 128)
                )
                for h in (2 * p, 2 * p + 1)
            ]
            value = local[at, lanes] + jnp.where(left_lanes, scale[0], scale[1]) * carried[:, lanes]
            out[at, lanes] = value.astype(BF16)
        return states[i] + jnp.exp(chunk_total(cum, i)) * state

    lax.fori_loop(0, 16, step, state, unroll=2)


def shards(
    grad_out, out_proj, step_size, log_decay, b_input, c_output,
    skip_gain, expert_ids, hidden_act, w_down,
):
    hidden = hidden_act[0].transpose(1, 0, 2).reshape(18, 8, 2, 16, 512)
    return pl.pallas_call(
        comm_kernel,
        name="mixer_and_router",
        out_shape=(
            jax.ShapeDtypeStruct((2048, 256), BF16),
            jax.ShapeDtypeStruct((2, 128), F32),
        ),
        in_specs=[HBM_ANY, HBM_ANY, VMEM_ANY, HBM_ANY, HBM_ANY] + [VMEM_ANY] * 5,
        out_specs=(VMEM_ANY, VMEM_ANY),
        scratch_shapes=[
            pltpu.VMEM((2048, 256), F32),
            pltpu.VMEM((8, 128, 2048), BF16),
            pltpu.VMEM((2, 256, 2048), BF16),
            pltpu.VMEM((8, 128, 256), F32),
            pltpu.VMEM((2304, 2048), BF16),
            pltpu.VMEM((144, 2048), BF16),
            pltpu.VMEM((2, 512, 2048), BF16),
            pltpu.VMEM((2, 18, 8, 16, 512), BF16),
            pltpu.VMEM((2, 2304, 512), BF16),
            pltpu.VMEM((16, 128), F32),
            pltpu.VMEM((9, 256), F32),
            pltpu.VMEM((8, 8, 128), F32),
            pltpu.VMEM((8, 8, 128), F32),
            pltpu.VMEM((16, 8, 128), F32),
            pltpu.VMEM((16, 8, 128), F32),
            pltpu.VMEM((16, 128, 8), F32),
            pltpu.VMEM((16, 128, 8), F32),
            pltpu.VMEM((16, 16, 256), F32),
            pltpu.VMEM((2, 24, 256), F32),
            pltpu.VMEM((8, 24, 256), F32),
            pltpu.SemaphoreType.DMA((160,)),
            pltpu.SemaphoreType.DMA((160,)),
            pltpu.SemaphoreType.DMA((4,)),
        ],
        compiler_params=pltpu.CompilerParams(
            collective_id=0, has_side_effects=True, vmem_limit_bytes=60 * 1024 * 1024
        ),
    )(
        grad_out, out_proj, expert_ids.T, hidden, w_down[0],
        log_decay, step_size, b_input, c_output, skip_gain.reshape(1, 256),
    )


def solution(mesh):
    in_specs = (
        P(("seq", "exp"), None),
        P("exp", None),
        P("exp", "seq"),
        P("exp", "seq"),
        P(None, "seq"),
        P(None, "seq"),
        P("exp"),
        P("seq", None),
        P("exp", None, None, "seq"),
        P("exp", "seq", None),
    )
    out_specs = (P("seq", "exp"), P(None, ("seq", "exp")))
    return jax.shard_map(shards, mesh=mesh, in_specs=in_specs, out_specs=out_specs, check_vma=False)
```

```python
import jax
import jax.numpy as jnp
from jax import lax
from jax.experimental import pallas as pl
from jax.experimental.pallas import tpu as pltpu
from jax.sharding import PartitionSpec as P

HEAD = 64
MESH = pl.DeviceIdType.MESH
F32, BF16 = jnp.float32, jnp.bfloat16

CAP = 18
HALF = (16, 32, 32, 32, 16, 16)
OFF = (0, 16, 48, 80, 112, 128)
BASE = (0, 256, 768, 1280, 1792, 2048)
CHUNKS = len(HALF)
RANK = (0, -1, 1, -2, 2, -3, 3, 4)
VMEM_ANY = pl.BlockSpec(memory_space=pltpu.VMEM)
HBM_ANY = pl.BlockSpec(memory_space=pl.ANY)


def dot_t(a, b):
    return lax.dot_general(a, b, (((1,), (1,)), ((), ())), preferred_element_type=F32)


def dot_n(a, b):
    return lax.dot_general(a, b, (((1,), (0,)), ((), ())), preferred_element_type=F32)


def dot_tn(a, b):
    return lax.dot_general(a, b, (((0,), (0,)), ((), ())), preferred_element_type=F32)


def halves(x):
    hi = x.astype(BF16)
    return hi, (x - hi.astype(F32)).astype(BF16)


def order_matrix(z, yl):
    row = lax.broadcasted_iota(jnp.int32, (288, 288), 0)
    col = lax.broadcasted_iota(jnp.int32, (288, 288), 1)
    late, last = row - 32, row - 224
    side = jnp.where(row < 32, row >> 4, jnp.where(row < 224, (late >> 5) & 1, (last >> 4) & 1))
    middle = jnp.where(
        row < 224, 16 + ((late >> 6) << 5) + (late & 31), 112 + ((last >> 5) << 4) + (last & 15)
    )
    place = jnp.where(row < 32, row & 15, middle)
    arrival = (place * 3641) >> 16
    slot = place - 18 * arrival
    shift = jnp.where((arrival & 1) == 1, -((arrival + 1) >> 1), arrival >> 1)
    source = (z + shift) & 7
    lane = jnp.where(side == 0, yl, 1 - yl)
    return col == slot * 16 + lane * 8 + source


def comm_kernel(
    g_hbm, w_hbm, ids, hid, wd_hbm, ld, st, b_in, c_in, gain, out, gate,
    inner, blocks, proj, outbox, rows, picks, wd, act, acts, keys, scores, sent, parts, tables,
    cum, cum_t, step_t, states, pair, chips, chosen, send, recv, local,
):
    s, e = lax.axis_index("seq"), lax.axis_index("exp")
    core, x, yh = s % 2, (s // 2) % 4, s // 8
    z, yl = e % 8, e // 8
    mine, other = yh * 4 + x, (1 - yh) * 4 + x
    plane = lambda yh_, x_: (yh_ * 4 + x_) * 2 + core
    zp, zm = (s, yl * 8 + (z + 1) % 8), (s, yl * 8 + (z + 7) % 8)
    xp, xm = (plane(yh, (x + 1) % 4), e), (plane(yh, (x + 3) % 4), e)
    yp, yq = (s, (1 - yl) * 8 + z), (plane(1 - yh, x), e)
    yd = (plane(1 - yh, x), (1 - yl) * 8 + z)
    sib = ((yh * 4 + x) * 2 + 1 - core, e)
    peers = (zp, zm, xp, xm, yp, yq, yd, sib)
    names, pending = {}, []

    def start(name, src, dst, to):
        i = names.setdefault(name, len(names))
        copy = pltpu.make_async_remote_copy(
            src_ref=src, dst_ref=dst, send_sem=send.at[i], recv_sem=recv.at[i],
            device_id=to, device_id_type=MESH,
        )
        copy.start()
        pending.append(copy)

    def arrived(name, dst):
        i = names[name]
        pltpu.make_async_remote_copy(
            src_ref=dst, dst_ref=dst, send_sem=send.at[i], recv_sem=recv.at[i],
            device_id=sib, device_id_type=MESH,
        ).wait_recv()

    def part(k, j, side=None):
        h = HALF[k]
        at = pl.multiple_of(BASE[k] + j * (2 * h), 2 * h)
        if side is None:
            return rows.at[pl.ds(at, 2 * h)]
        return rows.at[pl.ds(pl.multiple_of(at + side * h, 16), h)]

    spot = lambda a: (z + RANK[a] + 8) % 8
    loads = [
        pltpu.make_async_copy(g_hbm, blocks.at[z], local.at[0]),
        pltpu.make_async_copy(w_hbm, proj.at[yl], local.at[1]),
        pltpu.make_async_copy(wd_hbm, wd.at[core], local.at[2]),
        pltpu.make_async_copy(hid.at[:, :, core], act.at[core], local.at[3]),
    ]
    for load in loads:
        load.start()
    barrier = pltpu.get_barrier_semaphore()
    for peer in peers:
        pl.semaphore_signal(barrier, inc=1, device_id=peer, device_id_type=MESH)
    pl.semaphore_wait(barrier, len(peers))

    loads[0].wait()
    start("zp0", blocks.at[z], blocks.at[z], zp)
    start("zm0", blocks.at[z], blocks.at[z], zm)
    part_of_w = pl.ds(pl.multiple_of(core * 128, 128), 128)
    rest_of_w = pl.ds(pl.multiple_of((1 - core) * 128, 128), 128)
    loads[1].wait()
    start("wd", wd_hbm, wd.at[core], sib)
    start("hid", hid.at[:, :, 1 - core], act.at[core], sib)

    for a in range(8):
        lanes = pl.ds(pl.multiple_of((yl * 8 + spot(a)) * 128, 128), 128)
        named = ids[:, lanes]
        for side, expert in ((0, e), (1, (1 - yl) * 8 + z)):
            hit = (named[0:1] == expert) | (named[1:2] == expert)
            keys[2 * a + side : 2 * a + side + 1, :] = jnp.where(hit, 1.0, 0.0)
    hits = keys[...]
    tri = lax.broadcasted_iota(jnp.int32, (128, 128), 0) <= lax.broadcasted_iota(
        jnp.int32, (128, 128), 1
    )
    rank = dot_n(hits.astype(BF16), jnp.where(tri, 1.0, 0.0).astype(BF16))
    keys[...] = jnp.where(hits > 0.5, rank - 1.0, -1000.0)

    def pick(k):
        h = HALF[k]
        place = lax.broadcasted_iota(jnp.int32, (h, 128), 0) + OFF[k]
        first, last = OFF[k] // CAP, (OFF[k] + h - 1) // CAP
        wanted = []
        for a in range(first, last + 1):
            at = (place - CAP * a).astype(F32)
            sides = [keys[2 * a + side : 2 * a + side + 1, :] == at for side in (0, 1)]
            wanted.append(
                jnp.concatenate([jnp.where(m, 1.0, 0.0) for m in sides], axis=0).astype(BF16)
            )
        for n in range(0, 2048, 512):
            found = None
            for a, chosen in zip(range(first, last + 1), wanted):
                more = dot_n(chosen, blocks[spot(a), :, n : n + 512])
                found = more if found is None else found + more
            found = found.astype(BF16)
            at = pl.multiple_of(BASE[k] + mine * (2 * h), 2 * h)
            rows[pl.ds(at, h), n : n + 512] = found[:h]
            picks[OFF[k] : OFF[k] + h, n : n + 512] = found[h:]

    def pick_and_send(k):
        pick(k)
        cut = picks.at[OFF[k] : OFF[k] + HALF[k]]
        start(f"pl{k}", cut, part(k, mine, 1), yp)
        start(f"pd{k}", cut, part(k, mine, 1), yd)
        start(f"ow{k}", part(k, mine, 0), part(k, mine, 0), yq)
        to_both("a", k, mine, 0)

    def to_both(tag, k, j, side):
        start(f"xp{tag}{side}{k}", part(k, j, side), part(k, j, side), xp)
        start(f"xm{tag}{side}{k}", part(k, j, side), part(k, j, side), xm)

    def spread(k):
        arrived(f"pl{k}", part(k, mine, 1))
        to_both("a", k, mine, 1)
        arrived(f"pd{k}", part(k, other, 1))
        to_both("b", k, other, 1)
        arrived(f"ow{k}", part(k, other, 0))
        to_both("b", k, other, 0)

    def relay(k):
        for tag, side in (("a", yh), ("b", 1 - yh)):
            before, after = side * 4 + (x + 3) % 4, side * 4 + (x + 1) % 4
            arrived(f"xp{tag}0{k}", part(k, before, 0))
            start(f"fp{tag}{k}", part(k, before, 0), part(k, before, 0), xp)
            arrived(f"xm{tag}1{k}", part(k, after, 1))
            start(f"fm{tag}{k}", part(k, after, 1), part(k, after, 1), xm)

    def relayed(k):
        for tag, side in (("a", yh), ("b", 1 - yh)):
            before, after = side * 4 + (x + 3) % 4, side * 4 + (x + 1) % 4
            far = side * 4 + (x + 2) % 4
            arrived(f"xp{tag}1{k}", part(k, before, 1))
            arrived(f"xm{tag}0{k}", part(k, after, 0))
            arrived(f"fp{tag}{k}", part(k, far, 0))
            arrived(f"fm{tag}{k}", part(k, far, 1))

    def ring(k):
        back, ahead = (z - k + 8) % 8, (z + k) % 8
        if k < 4:
            arrived(f"zp{k - 1}", blocks.at[back])
            arrived(f"zm{k - 1}", blocks.at[ahead])
        else:
            arrived("zp3", blocks.at[back, 0:64])
            arrived("zm3", blocks.at[ahead, 64:128])
        if k < 3:
            start(f"zp{k}", blocks.at[back], blocks.at[back], zp)
            start(f"zm{k}", blocks.at[ahead], blocks.at[ahead], zm)
        elif k == 3:
            start("zp3", blocks.at[back, 0:64], blocks.at[back, 0:64], zp)
            start("zm3", blocks.at[ahead, 64:128], blocks.at[ahead, 64:128], zm)

    def product(a):
        block = blocks[spot(a)]
        outbox[a] = dot_t(block, proj[1 - yl])
        to = pl.ds(pl.multiple_of((yl * 8 + spot(a)) * 128, 128), 128)
        start(f"c{a}", outbox.at[a], inner.at[to], yp)
        inner[to, :] = dot_t(block, proj[yl])

    def ordered():
        loads[3].wait()
        arrived("hid", act.at[1 - core])
        matrix = jnp.where(order_matrix(z, yl), 1.0, 0.0).astype(BF16)

        def step(i, _):
            j, c = i // 2, i % 2
            source = act[c, :, j].reshape(288, 512)
            put = dot_n(matrix, source).astype(BF16)
            for k in range(CHUNKS):
                h = HALF[k]
                at = pl.multiple_of(BASE[k] + j * (2 * h), 2 * h)
                acts[c, pl.ds(at, 2 * h), :] = put[2 * OFF[k] : 2 * OFF[k] + 2 * h]
            return 0

        lax.fori_loop(0, 16, step, 0)

    def score(m):
        at = pl.multiple_of(m * 256, 256)
        lhs = rows[pl.ds(at, 256), :]

        def step(i, total):
            c, n = i // 2, pl.multiple_of((i % 2) * 256, 256)
            got = dot_t(lhs, wd[c, pl.ds(n, 256), :])
            prod = got * acts[c, pl.ds(at, 256), pl.ds(n, 256)].astype(F32)
            return total + prod[:, :128] + prod[:, 128:]

        total = lax.fori_loop(0, 4, step, jnp.zeros((256, 128), F32))
        scores[pl.ds(m, 1), :] = jnp.sum(total.T, axis=0, keepdims=True)

    def score_chunk(k):
        relayed(k)
        n, m = 2 * HALF[k], BASE[k] // 256
        if n == 32:
            score(m)
        else:
            lax.fori_loop(m, m + 2, lambda i, _: (score(i), 0)[1], 0)
        for j in range(8):
            at = n * j
            sent[j, k : k + 1, 0:n] = scores[m + at // 256 : m + at // 256 + 1, at % 256 : at % 256 + n]

    others = [(dy, dx) for dy in (0, 1) for dx in range(4) if dy or dx]
    toward = lambda dy, dx: ((yh + dy) % 2, (x + dx) % 4)

    def to_chips(tag, src_of, dst):
        for dy, dx in others:
            y_, x_ = toward(dy, dx)
            start(f"{tag}{dy}{dx}", src_of(y_ * 4 + x_), dst.at[mine], (plane(y_, x_), e))

    def from_chips(tag, dst):
        for dy, dx in others:
            y_, x_ = toward(dy, 4 - dx)
            arrived(f"{tag}{dy}{dx}", dst.at[y_ * 4 + x_])

    def chunk_of(a, side):
        shift = (a // 2) * (1 - 2 * (a % 2)) - a % 2
        return side * 8 + (z + shift + 8) % 8

    def own_part(first, last):
        for a in range(first, last):
            product(a)
        lax.fori_loop(first, last, lambda a, _: local_chunk(chunk_of(a, yl)), 0)

    def other_part(first, last):
        for a in range(first, last):
            to = pl.ds(pl.multiple_of(((1 - yl) * 8 + spot(a)) * 128, 128), 128)
            arrived(f"c{a}", inner.at[to])
        lax.fori_loop(first, last, lambda a, _: local_chunk(chunk_of(a, 1 - yl)), 0)

    def local_chunk(i):
        states[i] = chunk_state(inner, c_in, cum, i)
        within_chunk(inner, b_in, c_in, gain, cum, cum_t, step_t, i)
        return 0

    def summarize():
        total = shard_summary(states, cum)
        pair[core] = total
        start("pair", pair.at[core], pair.at[core], sib)

    def combine_pair():
        arrived("pair", pair.at[1 - core])
        grown = jnp.exp(pair[0, 16:17])
        chips[mine, 0:16] = pair[0, 0:16] + grown * pair[1, 0:16]
        chips[mine, 16:24] = pair[0, 16:24] + pair[1, 16:24]
        to_chips("st", lambda j: chips.at[mine], chips)

    def entering():
        from_chips("st", chips)

        def enter(n, state):
            k = 7 - n
            got = chips[k]
            return jnp.where(k > mine, got[0:16] + jnp.exp(got[16:17]) * state, state)

        state = lax.fori_loop(0, 8, enter, jnp.zeros((16, 256), F32))
        later = pair[1]
        return jnp.where(core == 0, later[0:16] + jnp.exp(later[16:17]) * state, state)

    def finish():
        to_chips("sc", lambda j: sent.at[j], parts)
        sweep(inner, b_in, out, cum, cum_t, step_t, states, entering())
        named = ids[:, pl.ds(pl.multiple_of(e * 128, 128), 128)]
        expert = lax.broadcasted_iota(jnp.int32, (16, 128), 0)
        hit = (named[0:1] == expert) | (named[1:2] == expert)
        lower = lax.broadcasted_iota(jnp.int32, (128, 128), 0)
        along = lax.broadcasted_iota(jnp.int32, (128, 128), 1)
        upto = jnp.where(lower <= along, 1.0, 0.0).astype(BF16)
        slot = dot_n(jnp.where(hit, 1.0, 0.0).astype(BF16), upto).astype(jnp.int32) - 1
        off = (z - (expert & 7) + 8) & 7
        place = 18 * jnp.where(off < 4, 2 * off, 15 - 2 * off) + slot
        wide = (place >= 16) & (place < 112)
        chunk = jnp.where(wide, 1 + ((place - 16) >> 5), jnp.where(place < 16, 0, 4 + ((place - 112) >> 4)))
        spot_ = jnp.where(wide, (place - 16) & 31, place & 15)
        lane = spot_ + jnp.where((expert >> 3) == yl, 0, jnp.where(wide, 32, 16))
        rows_of = []
        for k in (0, 1):
            for i in range(16):
                both = (lower == lane[i : i + 1]) & (named[k : k + 1] == i)
                chosen[k, 128 * i : 128 * i + 128, :] = jnp.where(both, 1.0, 0.0).astype(BF16)
            own = jnp.where(expert == named[k : k + 1], chunk, 0)
            rows_of.append(jnp.sum(own, axis=0, keepdims=True))
        from_chips("sc", parts)
        total = sent[mine]
        for dy, dx in others:
            y_, x_ = toward(dy, dx)
            total = total + parts[y_ * 4 + x_]
        tables[e] = total
        for d in range(1, 16):
            start(f"ex{d}", tables.at[e], tables.at[e], (s, (e + d) % 16))
        for d in range(1, 16):
            arrived(f"ex{d}", tables.at[(e + 16 - d) % 16])
        row8 = lax.broadcasted_iota(jnp.int32, (8, 128), 0)
        table = jnp.concatenate([tables[i] for i in range(16)], axis=1)
        hi = table.astype(BF16)
        mid, low = halves(table - hi.astype(F32))
        thirds = jnp.concatenate([v.astype(F32) for v in (hi, mid, low)], axis=0).astype(BF16)
        lines = []
        for k in (0, 1):
            got = dot_n(thirds, chosen[k])
            got = (got[16:24] + got[8:16]) + got[0:8]
            lines.append(jnp.sum(jnp.where(row8 == rows_of[k], got, 0.0), axis=0, keepdims=True))
        gate[...] = jnp.concatenate(lines, axis=0)

    def send_w(n):
        at = pl.ds(pl.multiple_of(core * 128 + 64 * n, 64), 64)
        start(f"w{n}", proj.at[yl, at], proj.at[yl, at], yd)

    pick_and_send(0)
    send_w(0)
    sent[...] = jnp.zeros_like(sent)
    spread(0)
    chunk_decays(ld, cum, cum_t)
    turn_steps(st, step_t)
    ring(1)
    pick_and_send(1)
    send_w(1)
    ordered()
    spread(1)
    ring(2)
    pick_and_send(2)
    for n in (0, 1):
        arrived(f"w{n}", proj.at[1 - yl, pl.ds(pl.multiple_of(core * 128 + 64 * n, 64), 64)])
    start("wf", proj.at[1 - yl, part_of_w], proj.at[1 - yl, part_of_w], sib)
    relay(0)
    spread(2)
    arrived("wf", proj.at[1 - yl, rest_of_w])
    own_part(0, 3)
    ring(3)
    pick_and_send(3)
    relay(1)
    spread(3)
    own_part(3, 5)
    ring(4)
    pick_and_send(4)
    pick_and_send(5)
    spread(4)
    spread(5)
    own_part(5, 8)
    other_part(0, 3)
    relay(2)
    other_part(3, 5)
    loads[2].wait()
    arrived("wd", wd.at[1 - core])
    score_chunk(0)
    score_chunk(1)
    relay(3)
    other_part(5, 8)
    summarize()
    score_chunk(2)
    combine_pair()
    relay(4)
    relay(5)
    score_chunk(3)
    score_chunk(4)
    score_chunk(5)
    finish()
    for copy in pending:
        copy.wait_send()


def chunk_decays(ld, cum, cum_t):
    lines = [
        jnp.concatenate([ld[:, 128 * i : 128 * (i + 1)], jnp.zeros((4, 128), F32)], axis=0)
        for i in range(16)
    ]
    x = jnp.concatenate(lines, axis=0)
    hi, rest = x.astype(BF16), None
    rest = x - hi.astype(F32)
    mid, low = halves(rest)
    tri = lax.broadcasted_iota(jnp.int32, (128, 128), 0) <= lax.broadcasted_iota(
        jnp.int32, (128, 128), 1
    )
    tri = jnp.where(tri, 1.0, 0.0).astype(BF16)
    total = (dot_n(low, tri) + dot_n(mid, tri)) + dot_n(hi, tri)
    for i in range(16):
        cum[i] = total[8 * i : 8 * i + 8]
    if cum_t is not None:
        turned = total.T
        for i in range(16):
            cum_t[i] = turned[:, 8 * i : 8 * i + 8]


def by_head(values):
    lane = lax.broadcasted_iota(jnp.int32, (1, 256), 1) // HEAD
    out = jnp.broadcast_to(values[3], (1, 256))
    for i in (2, 1, 0):
        out = jnp.where(lane == i, jnp.broadcast_to(values[i], (1, 256)), out)
    return out


def chunk_state(inner, c_in, cum, i):
    at = pl.ds(pl.multiple_of(i * 128, 128), 128)
    grown = jnp.exp(cum[i])
    c = c_in[:, at]
    hi, low = halves(jnp.concatenate([c * grown[h : h + 1] for h in range(4)], axis=0))
    g_hi, g_low = halves(inner[at, :])
    left = jnp.concatenate([hi, low, hi], axis=1)
    right = jnp.concatenate([g_hi, g_hi, g_low], axis=0)
    full = dot_n(left, right)
    lane = lax.broadcasted_iota(jnp.int32, (16, 256), 1) // HEAD
    out = full[48:64]
    for h in (2, 1, 0):
        out = jnp.where(lane == h, full[16 * h : 16 * h + 16], out)
    return out


def chunk_total(cum, i):
    ends = cum[i]
    return by_head([ends[h : h + 1, 127:128] for h in range(4)])


def shard_summary(states, cum):
    def step(n, carry):
        state, total = carry
        ends = chunk_total(cum, 15 - n)
        return states[15 - n] + jnp.exp(ends) * state, total + ends

    state, total = lax.fori_loop(
        0, 16, step, (jnp.zeros((16, 256), F32), jnp.zeros((1, 256), F32)), unroll=4
    )
    return jnp.concatenate([state, jnp.broadcast_to(total, (8, 256))], axis=0)


def turn_steps(st, step_t):
    lines = [
        jnp.concatenate([st[:, 128 * i : 128 * (i + 1)], jnp.zeros((4, 128), F32)], axis=0)
        for i in range(16)
    ]
    turned = jnp.concatenate(lines, axis=0).T
    for i in range(16):
        step_t[i] = turned[:, 8 * i : 8 * i + 8]


def within_chunk(inner, b_in, c_in, gain, cum, cum_t, step_t, i):
    upper = lax.broadcasted_iota(jnp.int32, (128, 128), 1) >= lax.broadcasted_iota(
        jnp.int32, (128, 128), 0
    )
    left_lanes = lax.broadcasted_iota(jnp.int32, (128, 128), 1) < HEAD
    gains = gain[...]
    at = pl.ds(pl.multiple_of(i * 128, 128), 128)
    b_hi, b_low = halves(b_in[:, at])
    c_hi, c_low = halves(c_in[:, at])
    b_all = jnp.concatenate([b_hi, b_low, b_hi], axis=0)
    table = dot_tn(b_all, jnp.concatenate([c_hi, c_hi, c_low], axis=0))
    rows_, cols, steps = cum[i], cum_t[i], step_t[i]
    for p in (0, 1):
        lanes = slice(128 * p, 128 * p + 128)
        g = inner[at, lanes]
        size, m_hi, m_low = [], [], []
        for h in (2 * p, 2 * p + 1):
            col = jnp.broadcast_to(cols[:, h : h + 1], (128, 128))
            gap = jnp.where(upper, rows_[h : h + 1] - col, 0.0)
            weight = jnp.where(upper, jnp.exp(gap), 0.0) * table
            hi, low = halves(weight)
            m_hi.append(hi)
            m_low.append(low)
            size.append(jnp.broadcast_to(steps[:, h : h + 1], (128, 128)))
        g_a, g_b = halves(jnp.where(left_lanes, g, 0.0)), halves(jnp.where(left_lanes, 0.0, g))
        left = jnp.concatenate(m_hi + m_low + m_hi, axis=1)
        right = jnp.concatenate([g_a[0], g_b[0], g_a[0], g_b[0], g_a[1], g_b[1]], axis=0)
        sizes = jnp.where(left_lanes, size[0], size[1])
        inner[at, lanes] = sizes * dot_n(left, right) + gains[:, lanes] * g


def sweep(local, b_in, out, cum, cum_t, step_t, states, state):
    left_lanes = lax.broadcasted_iota(jnp.int32, (128, 128), 1) < HEAD

    def step(n, state):
        i = 15 - n
        at = pl.ds(pl.multiple_of(i * 128, 128), 128)
        b_hi, b_low = halves(b_in[:, at])
        s_hi, s_low = halves(state)
        carried = dot_tn(
            jnp.concatenate([b_hi, b_low, b_hi], axis=0),
            jnp.concatenate([s_hi, s_hi, s_low], axis=0),
        )
        ends, cols, steps = cum[i][:, 127:128], cum_t[i], step_t[i]
        for p in (0, 1):
            lanes = slice(128 * p, 128 * p + 128)
            scale = [
                jnp.broadcast_to(
                    steps[:, h : h + 1] * jnp.exp(ends[h : h + 1] - cols[:, h : h + 1]), (128, 128)
                )
                for h in (2 * p, 2 * p + 1)
            ]
            value = local[at, lanes] + jnp.where(left_lanes, scale[0], scale[1]) * carried[:, lanes]
            out[at, lanes] = value.astype(BF16)
        return states[i] + jnp.exp(chunk_total(cum, i)) * state

    lax.fori_loop(0, 16, step, state, unroll=2)


def hand_over(d_in, gate_in, d_out, gate_out):
    d_out[...] = d_in[...]
    gate_out[...] = gate_in[...]


def shards(
    grad_out, out_proj, step_size, log_decay, b_input, c_output,
    skip_gain, expert_ids, hidden_act, w_down,
):
    hidden = hidden_act[0].transpose(1, 0, 2).reshape(18, 8, 2, 16, 512)
    results = pl.pallas_call(
        comm_kernel,
        name="mixer_and_router",
        out_shape=(
            jax.ShapeDtypeStruct((2048, 256), BF16),
            jax.ShapeDtypeStruct((2, 128), F32),
        ),
        in_specs=[HBM_ANY, HBM_ANY, VMEM_ANY, HBM_ANY, HBM_ANY] + [VMEM_ANY] * 5,
        out_specs=(VMEM_ANY, VMEM_ANY),
        scratch_shapes=[
            pltpu.VMEM((2048, 256), F32),
            pltpu.VMEM((8, 128, 2048), BF16),
            pltpu.VMEM((2, 256, 2048), BF16),
            pltpu.VMEM((8, 128, 256), F32),
            pltpu.VMEM((2304, 2048), BF16),
            pltpu.VMEM((144, 2048), BF16),
            pltpu.VMEM((2, 512, 2048), BF16),
            pltpu.VMEM((2, 18, 8, 16, 512), BF16),
            pltpu.VMEM((2, 2304, 512), BF16),
            pltpu.VMEM((16, 128), F32),
            pltpu.VMEM((9, 256), F32),
            pltpu.VMEM((8, 8, 128), F32),
            pltpu.VMEM((8, 8, 128), F32),
            pltpu.VMEM((16, 8, 128), F32),
            pltpu.VMEM((16, 8, 128), F32),
            pltpu.VMEM((16, 128, 8), F32),
            pltpu.VMEM((16, 128, 8), F32),
            pltpu.VMEM((16, 16, 256), F32),
            pltpu.VMEM((2, 24, 256), F32),
            pltpu.VMEM((8, 24, 256), F32),
            pltpu.VMEM((2, 2048, 128), BF16),
            pltpu.SemaphoreType.DMA((160,)),
            pltpu.SemaphoreType.DMA((160,)),
            pltpu.SemaphoreType.DMA((4,)),
        ],
        compiler_params=pltpu.CompilerParams(
            collective_id=0, has_side_effects=True, vmem_limit_bytes=60 * 1024 * 1024
        ),
    )(
        grad_out, out_proj, expert_ids.T, hidden, w_down[0],
        log_decay, step_size, b_input, c_output, skip_gain.reshape(1, 256),
    )
    return pl.pallas_call(
        hand_over,
        name="hand_over",
        out_shape=(
            jax.ShapeDtypeStruct((2048, 256), BF16),
            jax.ShapeDtypeStruct((2, 128), F32),
        ),
        in_specs=[VMEM_ANY] * 2,
        out_specs=(VMEM_ANY, VMEM_ANY),
    )(*results)


def solution(mesh):
    in_specs = (
        P(("seq", "exp"), None),
        P("exp", None),
        P("exp", "seq"),
        P("exp", "seq"),
        P(None, "seq"),
        P(None, "seq"),
        P("exp"),
        P("seq", None),
        P("exp", None, None, "seq"),
        P("exp", "seq", None),
    )
    out_specs = (P("seq", "exp"), P(None, ("seq", "exp")))
    return jax.shard_map(shards, mesh=mesh, in_specs=in_specs, out_specs=out_specs, check_vma=False)
```
